128 devices in a mesh: node: 8 (over x, core), local: 16 (over y, z).
Axes of the slice: x: 4, y: 4, z: 4, core: 2. Of those that a mesh axis runs over, the one named last changes fastest.
Arguments:
- tokens: bfloat16 [8192, 7168], P(('node', 'local')), may hold values from -6 to 6
- routes: int32 [8192, 2], P(('node', 'local')), may hold values from 0 to 31, as said below
- scores: float32 [8192, 2], P(('node', 'local')), may hold values from 0.1 to 1
- gate_proj: bfloat16 [128, 7168, 512], P(('node', 'local')), may hold values from -0.0625 to 0.0625
- up_proj: bfloat16 [128, 7168, 512], P(('node', 'local')), may hold values from -0.0625 to 0.0625
- down_proj: bfloat16 [128, 512, 7168], P(('node', 'local')), may hold values from -0.125 to 0.125
Outputs:
- combined: bfloat16 [8192, 7168], P(('node', 'local'))
The draws below stay inside these ranges and needn't reach their ends.
Inputs may be any that keep to these rules, and one draw needn't show every extreme that they name: `routes`: each row names 2 different experts. The rows of one device name each expert at most 5 times, and in every draw one expert is named by exactly 5 rows of every device.
All inputs are finite; a program needn't handle non-finite values.
Results may differ from the reference program's by a relative error of at most 0.0085.
Values may be sent and summed in bfloat16 or wider, within the bound.
A program may use at most 192 MiB of HBM per device.

```python
import math
import jax
import jax.numpy as jnp
from jax import lax

D = 7168
FF = 2048
SHARDS = 4
TOP = 2
TOK_DEV = 64
FF_DEV = 512
EXPERTS = 32
MOST = 5
TOKENS = 8192


def draw_routes(key, part):
    blocks = TOKENS // TOK_DEV
    base_key = jax.random.fold_in(key, 11)
    key_hot, key_cycle, key_perm, key_order = jax.random.split(base_key, 4)
    hot_expert = jax.random.randint(key_hot, (), 0, EXPERTS)
    cycle_least = max(TOP, (TOK_DEV * TOP - MOST + MOST - 1) // MOST)
    cycle_length = jax.random.randint(key_cycle, (blocks,), cycle_least, EXPERTS)
    shuffles = jax.vmap(lambda one_key: jax.random.permutation(one_key, EXPERTS - 1))(jax.random.split(key_perm, blocks))
    others = shuffles + (shuffles >= hot_expert).astype(shuffles.dtype)
    token_ids = jnp.arange(TOK_DEV)[:, None]
    slot_ids = jnp.arange(TOP)[None, :]
    leading = token_ids < MOST
    other_pos = jnp.where(leading, token_ids * (TOP - 1) + slot_ids - 1, MOST * (TOP - 1) + (token_ids - MOST) * TOP + slot_ids)
    cycle_pos = jnp.mod(other_pos[None, :, :], cycle_length[:, None, None])
    chosen = jnp.take_along_axis(others, cycle_pos.reshape(blocks, -1), axis=1).reshape(blocks, TOK_DEV, TOP)
    chosen = jnp.where((leading & (slot_ids == 0))[None, :, :], hot_expert, chosen)
    token_order = jax.vmap(lambda one_key: jax.random.permutation(one_key, TOK_DEV))(jax.random.split(key_order, blocks))
    chosen = jnp.take_along_axis(chosen, token_order[:, :, None], axis=1)
    return chosen.reshape(TOKENS, TOP).astype(jnp.int32)


def shard_levels(stream_key, shape, shards, low, largest):
    factor_of, own = 1.0, jax.random.fold_in(stream_key, 6)
    for position, shards_of in shards:
        draws = jnp.exp(jax.random.uniform(jax.random.fold_in(own, position), (shards_of,), jnp.float32, low / len(shards), largest / len(shards)))
        factor_of = factor_of * jnp.repeat(draws, shape[position] // shards_of).reshape([-1 if axis == position else 1 for axis in range(len(shape))])
    return factor_of


def noise(stream_key, dims, spread, bound, pieces=(), kind=jnp.bfloat16):
    level = shard_levels(stream_key, dims, pieces, -0.22, 0.18) if pieces else 1.0
    entries = jax.random.normal(stream_key, dims, jnp.float32) * spread * level
    return jnp.minimum(jnp.maximum(entries, -bound), bound).astype(kind)


def setup_inputs(seed: int = 0) -> dict:
    splits = jax.random.split(jax.random.key(seed), 7)
    return {
        "tokens": noise(splits[0], (TOKENS, D), 1.0, 6.0, ((0, 128),)),
        "routes": draw_routes(jax.random.fold_in(splits[6], 71), 0),
        "scores": jnp.clip(jnp.exp(math.log(1.0) - 2.3025851 * jax.random.uniform(splits[2], (TOKENS, TOP), jnp.float32) ** shard_levels(splits[2], (TOKENS, TOP), ((0, 128),), -0.2, 0.2)), 0.1, 1.0),
        "gate_proj": noise(splits[3], (EXPERTS * SHARDS, D, FF_DEV), D ** -0.5, 0.0625, ((0, 128),)),
        "up_proj": noise(splits[4], (EXPERTS * SHARDS, D, FF_DEV), D ** -0.5, 0.0625, ((0, 128),)),
        "down_proj": noise(splits[5], (EXPERTS * SHARDS, FF_DEV, D), FF ** -0.5, 0.125, ((0, 128),)),
    }


SCALE = 2.827


def reference(tokens, routes, scores, gate_proj, up_proj, down_proj):
    pair_count = TOKENS * TOP
    weights = (SCALE * scores / jnp.sum(scores, axis=1, keepdims=True)).astype(jnp.bfloat16)
    flat_exp = routes.reshape(-1).astype(jnp.int32)
    sort_order = jnp.argsort(flat_exp, stable=True).astype(jnp.int32)
    labels = jnp.arange(EXPERTS, dtype=jnp.int32)
    counts = jnp.sum((flat_exp[:, None] == labels[None, :]).astype(jnp.int32), axis=0).astype(jnp.int32)
    padded = (((counts + 127) // 128) * 128).astype(jnp.int32)
    group_ends = jnp.cumsum(padded).astype(jnp.int32)
    group_starts = (group_ends - padded).astype(jnp.int32)
    sorted_starts = (jnp.cumsum(counts) - counts).astype(jnp.int32)
    sorted_exp = flat_exp[sort_order]
    rank_list = jnp.arange(pair_count, dtype=jnp.int32)
    target_pos = (group_starts[sorted_exp] + rank_list - sorted_starts[sorted_exp]).astype(jnp.int32)
    block_count = (pair_count + 127) // 128 + EXPERTS
    slot_table = jnp.full((block_count * 128,), pair_count, jnp.int32).at[target_pos].set(sort_order)
    block_first = jnp.arange(block_count, dtype=jnp.int32) * 128
    block_exp = jnp.minimum(jnp.sum((group_ends[None, :] <= block_first[:, None]).astype(jnp.int32), axis=1), EXPERTS - 1).astype(jnp.int32)
    pair_weight = jnp.concatenate([weights.reshape(-1).astype(jnp.float32), jnp.zeros((1,), jnp.float32)])
    padded_x = jnp.concatenate([tokens, jnp.zeros((1, D), jnp.bfloat16)], axis=0)

    def accumulate(running, block_num):
        row_index = lax.dynamic_slice_in_dim(slot_table, (block_num * 128).astype(jnp.int32), 128)
        token_index = (row_index // TOP).astype(jnp.int32)
        expert = block_exp[block_num]
        row_data = padded_x[token_index]
        row_weight = pair_weight[row_index]
        first_row = (expert * SHARDS).astype(jnp.int32)
        w_gate = lax.dynamic_slice_in_dim(gate_proj, first_row, SHARDS, 0).transpose(1, 0, 2).reshape(D, FF)
        w_up = lax.dynamic_slice_in_dim(up_proj, first_row, SHARDS, 0).transpose(1, 0, 2).reshape(D, FF)
        gate_act = jnp.dot(row_data, w_gate, preferred_element_type=jnp.float32)
        up_act = jnp.dot(row_data, w_up, preferred_element_type=jnp.float32)
        hidden = (jax.nn.silu(gate_act) * up_act).astype(jnp.bfloat16)
        w_down = lax.dynamic_slice_in_dim(down_proj, first_row, SHARDS, 0)
        summed = jnp.zeros((128, D), jnp.float32)
        for shard_num in range(SHARDS):
            partial_value = jnp.dot(hidden[:, shard_num * FF_DEV:(shard_num + 1) * FF_DEV], w_down[shard_num], preferred_element_type=jnp.float32).astype(jnp.bfloat16)
            summed = summed + partial_value.astype(jnp.float32)
        running = running.at[token_index].add(summed * row_weight[:, None])
        return running, None

    running = lax.scan(accumulate, jnp.zeros((TOKENS + 1, D), jnp.float32), jnp.arange(block_count, dtype=jnp.int32))[0]
    return running[:TOKENS].astype(jnp.bfloat16)
```

```python
import functools

import jax
import jax.numpy as jnp
from jax import lax
from jax.experimental import pallas as pl
from jax.experimental.pallas import tpu as pltpu
from jax.sharding import PartitionSpec as P

MESH = pl.DeviceIdType.MESH
SHARDS = 4
SCALE = 2.827
MOST = 5
LANES = 128


def kernel(
    plane, rows_of, wide,
    pick_ref, home_ref, weight_ref, tok_ref, gate_hbm, up_hbm, down_hbm,
    out_ref,
    w_gate, w_up, w_down, sent, got, x_all, part, half_in, full_in, back, home, wide32, acc, hid,
    w_sem, plane_s, plane_r, ag_s, ag_r, fw_s, fw_r, rh_s, rh_r, rf_s, rf_r, back_s, back_r,
):
    node, local = lax.axis_index("node"), lax.axis_index("local")
    ys = lax.axis_size("local") // SHARDS
    y, z = local // SHARDS, local % SHARDS
    me = node * ys + y
    nxt, prv, far = (z + 1) % SHARDS, (z + 3) % SHARDS, (z + 2) % SHARDS
    up_dev = (node, y * SHARDS + nxt)
    dn_dev = (node, y * SHARDS + prv)
    subs = wide // LANES
    half = plane // 2
    depth = w_gate.shape[0]
    hidden = w_gate.shape[1]

    w_copies = [
        pltpu.make_async_copy(gate_hbm.at[0], w_gate, w_sem.at[0]),
        pltpu.make_async_copy(up_hbm.at[0], w_up, w_sem.at[1]),
        pltpu.make_async_copy(down_hbm.at[0], w_down, w_sem.at[2]),
    ]
    for copy in w_copies:
        copy.start()

    def peer(k):
        other = lax.rem(me + k, plane)
        return other, (other // ys, (other % ys) * SHARDS + z)

    barrier = pltpu.get_barrier_semaphore()

    def greet(k, carry):
        pl.semaphore_signal(barrier, inc=1, device_id=peer(k)[1], device_id_type=MESH)
        return carry

    lax.fori_loop(1, plane, greet, 0)
    for dev in (up_dev, dn_dev):
        pl.semaphore_signal(barrier, inc=1, device_id=dev, device_id_type=MESH)

    def fill(i, carry):
        c, e = i // plane, i % plane
        sent[c, e] = tok_ref[pick_ref[c, e]]
        return carry

    lax.fori_loop(0, rows_of * plane, fill, 0)
    pl.semaphore_wait(barrier, plane + 1)

    def remote(src, dst, s_sem, r_sem, dev):
        return pltpu.make_async_remote_copy(
            src_ref=src, dst_ref=dst, send_sem=s_sem, recv_sem=r_sem, device_id=dev, device_id_type=MESH
        )

    def spread(src, dst, s_sem, r_sem, c):
        def one(k, carry):
            other, dev = peer(k)
            remote(src.at[c, other], dst.at[c, me], s_sem.at[c], r_sem.at[c], dev).start()
            return carry

        lax.fori_loop(1, plane, one, 0)
        dst[c, me] = src[c, me]

    def spread_all(src, dst, s_sem, r_sem, c):
        some = pl.ds(0, plane - 1)
        return remote(src.at[c, some], dst.at[c, some], s_sem.at[c], r_sem.at[c], up_dev)

    def gather(c):
        return (
            remote(x_all.at[c, z], x_all.at[c, z], ag_s.at[c, 0], ag_r.at[c, 0], up_dev),
            remote(x_all.at[c, z], x_all.at[c, z], ag_s.at[c, 1], ag_r.at[c, 1], dn_dev),
        )

    def forward(c):
        low, high = pl.ds(0, half), pl.ds(half, half)
        return (
            remote(x_all.at[c, prv, low], x_all.at[c, prv, low], fw_s.at[c, 0], fw_r.at[c, 0], up_dev),
            remote(x_all.at[c, nxt, high], x_all.at[c, nxt, high], fw_s.at[c, 1], fw_r.at[c, 1], dn_dev),
        )

    def scatter_half(c):
        low, high = pl.ds(0, half), pl.ds(half, half)
        return (
            remote(part.at[c, far, low], half_in.at[c, 0], rh_s.at[c, 0], rh_r.at[c, 0], up_dev),
            remote(part.at[c, far, high], half_in.at[c, 1], rh_s.at[c, 1], rh_r.at[c, 1], dn_dev),
        )

    def scatter_full(c):
        return (
            remote(part.at[c, nxt], full_in.at[c, 0], rf_s.at[c, 0], rf_r.at[c, 0], up_dev),
            remote(part.at[c, prv], full_in.at[c, 1], rf_s.at[c, 1], rf_r.at[c, 1], dn_dev),
        )

    def stage_a(c):
        spread_all(sent, got, plane_s, plane_r, c).wait_recv()

        def widen(s, carry):
            wide32[pl.ds(pl.multiple_of(s * subs, 8), subs), :] = got[c, s].astype(jnp.float32)
            return carry

        lax.fori_loop(0, plane, widen, 0)

        def column(j, carry):
            cols = pl.ds(pl.multiple_of(j * LANES, LANES), LANES)
            for s0 in range(0, plane, 16):
                rows = [wide32[pl.ds((s0 + d) * subs + j, 8, stride=subs), :] for d in (0, 8)]
                x_all[c, z, pl.ds(s0, 16), cols] = jnp.concatenate(rows, axis=0).astype(jnp.bfloat16)
            return carry

        lax.fori_loop(0, subs, column, 0)
        for copy in gather(c):
            copy.start()

    def stage_b(c):
        for copy in gather(c):
            copy.wait_recv()
        for copy in forward(c):
            copy.start()

    def stage_c(c):
        for copy in forward(c):
            copy.wait_recv()
        rows = SHARDS * plane
        block = min(1024, depth)

        acc[...] = jnp.zeros_like(acc)

        def contract(k, carry):
            span = pl.ds(pl.multiple_of(k * block, LANES), block)
            rows_k = x_all[c, :, :, span].reshape(rows, block)
            acc[:, :hidden] += jnp.dot(rows_k, w_gate[span, :], preferred_element_type=jnp.float32)
            acc[:, hidden:] += jnp.dot(rows_k, w_up[span, :], preferred_element_type=jnp.float32)
            return carry

        lax.fori_loop(0, depth // block, contract, 0)
        gate = acc[:, :hidden]
        hid[...] = (gate / (1.0 + jnp.exp(-gate)) * acc[:, hidden:]).astype(jnp.bfloat16)

        def expand(k, carry):
            span = pl.ds(pl.multiple_of(k * block, LANES), block)
            value = jnp.dot(hid[...], w_down[:, span], preferred_element_type=jnp.float32)
            part[c, :, :, span] = value.astype(jnp.bfloat16).reshape(SHARDS, plane, block)
            return carry

        lax.fori_loop(0, depth // block, expand, 0)
        for copy in scatter_half(c):
            copy.start()

    def stage_e(c):
        for copy in scatter_half(c):
            copy.wait_recv()
        for side, owner, start in ((0, nxt, 0), (1, prv, half)):
            span = pl.ds(start, half)
            mine = part[c, owner, span].astype(jnp.float32)
            part[c, owner, span] = (mine + half_in[c, side].astype(jnp.float32)).astype(jnp.bfloat16)
        for copy in scatter_full(c):
            copy.start()

    def stage_f(c):
        for copy in scatter_full(c):
            copy.wait_recv()

        def column(j, carry):
            cols = pl.ds(pl.multiple_of(j * LANES, LANES), LANES)
            for s0 in range(0, plane, 16):
                span = pl.ds(s0, 16)
                value = part[c, z, span, cols].astype(jnp.float32)
                value = value + full_in[c, 0, span, cols].astype(jnp.float32)
                value = value + full_in[c, 1, span, cols].astype(jnp.float32)
                for d in (0, 8):
                    wide32[pl.ds((s0 + d) * subs + j, 8, stride=subs), :] = value[d:d + 8]
            return carry

        lax.fori_loop(0, subs, column, 0)

        def narrow(s, carry):
            back[c, s] = wide32[pl.ds(pl.multiple_of(s * subs, 8), subs), :].astype(jnp.bfloat16)
            return carry

        lax.fori_loop(0, plane, narrow, 0)
        spread(back, home, back_s, back_r, c)

    def launch(c, carry):
        spread(sent, got, plane_s, plane_r, c)
        return carry

    lax.fori_loop(0, rows_of, launch, 0)

    stages = (stage_a, stage_b, stage_c, stage_e, stage_f)

    def step(s, carry):
        @pl.when(s == 2)
        def _():
            for copy in w_copies:
                copy.wait()

        for lag, stage in enumerate(stages):
            c = s - lag

            @pl.when((c >= 0) & (c < rows_of))
            def _(stage=stage, c=c):
                stage(c)

        return carry

    lax.fori_loop(0, rows_of + len(stages) - 1, step, 0)

    def arrive(c, carry):
        spread_all(back, home, back_s, back_r, c).wait_recv()
        return carry

    lax.fori_loop(0, rows_of, arrive, 0)

    def combine(t, carry):
        total = jnp.zeros((subs, LANES), jnp.float32)
        for k in range(home_ref.shape[1]):
            spot = home_ref[t, k]
            total = total + weight_ref[t, k] * home[spot // plane, spot % plane].astype(jnp.float32)
        out_ref[t] = total.astype(jnp.bfloat16)
        return carry

    lax.fori_loop(0, out_ref.shape[0], combine, 0)

    def drain(c, carry):
        spread_all(sent, got, plane_s, plane_r, c).wait_send()
        spread_all(back, home, back_s, back_r, c).wait_send()
        for group in (gather, forward, scatter_half, scatter_full):
            for copy in group(c):
                copy.wait_send()
        return carry

    lax.fori_loop(0, rows_of, drain, 0)


def per_device(tokens, routes, scores, gate_proj, up_proj, down_proj):
    plane = lax.axis_size("node") * (lax.axis_size("local") // SHARDS)
    count, wide = tokens.shape
    depth, hidden = gate_proj.shape[1:]
    subs = wide // LANES
    weights = (SCALE * scores / jnp.sum(scores, axis=1, keepdims=True)).astype(jnp.bfloat16).astype(jnp.float32)
    labels = jnp.arange(plane, dtype=jnp.int32)
    matches = routes[:, :, None] == labels[None, None, :]
    named = jnp.any(matches, axis=1)
    earlier = jnp.arange(count)[:, None] > jnp.arange(count)[None, :]
    rank = jnp.sum(earlier[:, :, None] & named[None], axis=1, dtype=jnp.int32)
    slots = jnp.arange(MOST, dtype=jnp.int32)
    chosen = named[None] & (rank[None] == slots[:, None, None])
    pick = jnp.sum(jnp.where(chosen, jnp.arange(count, dtype=jnp.int32)[None, :, None], 0), axis=1)
    home = jnp.sum(jnp.where(matches, rank[:, None, :] * plane + labels[None, None, :], 0), axis=2)
    bf16, f32 = jnp.bfloat16, jnp.float32
    dma = pltpu.SemaphoreType.DMA
    vmem, smem, hbm = pltpu.VMEM, pltpu.SMEM, pl.ANY
    out = pl.pallas_call(
        functools.partial(kernel, plane, MOST, wide),
        out_shape=jax.ShapeDtypeStruct((count, subs, LANES), bf16),
        in_specs=[pl.BlockSpec(memory_space=m) for m in (smem, smem, smem, vmem, hbm, hbm, hbm)],
        out_specs=pl.BlockSpec(memory_space=vmem),
        scratch_shapes=[
            vmem((depth, hidden), bf16),
            vmem((depth, hidden), bf16),
            vmem((hidden, depth), bf16),
            vmem((MOST, plane, subs, LANES), bf16),
            vmem((MOST, plane, subs, LANES), bf16),
            vmem((MOST, SHARDS, plane, wide), bf16),
            vmem((MOST, SHARDS, plane, wide), bf16),
            vmem((MOST, 2, plane // 2, wide), bf16),
            vmem((MOST, 2, plane, wide), bf16),
            vmem((MOST, plane, subs, LANES), bf16),
            vmem((MOST, plane, subs, LANES), bf16),
            vmem((plane * subs, LANES), f32),
            vmem((SHARDS * plane, 2 * hidden), f32),
            vmem((SHARDS * plane, hidden), bf16),
            dma((3,)),
            dma((MOST,)), dma((MOST,)),
            dma((MOST, 2)), dma((MOST, 2)),
            dma((MOST, 2)), dma((MOST, 2)),
            dma((MOST, 2)), dma((MOST, 2)),
            dma((MOST, 2)), dma((MOST, 2)),
            dma((MOST,)), dma((MOST,)),
        ],
        compiler_params=pltpu.CompilerParams(
            collective_id=0, has_side_effects=True, vmem_limit_bytes=67043328
        ),
    )(pick, home, weights, tokens.reshape(count, subs, LANES), gate_proj, up_proj, down_proj)
    return out.reshape(count, wide)


def solution(mesh):
    both = ("node", "local")
    return jax.shard_map(
        per_device,
        mesh=mesh,
        in_specs=(P(both, None),) * 3 + (P(both, None, None),) * 3,
        out_specs=P(both, None),
        check_vma=False,
    )
```

```python
import functools

import jax
import jax.numpy as jnp
from jax import lax
from jax.experimental import pallas as pl
from jax.experimental.pallas import tpu as pltpu
from jax.sharding import PartitionSpec as P

MESH = pl.DeviceIdType.MESH
SHARDS = 4
SCALE = 2.827
MOST = 5
LANES = 128
LATE_IN = 2
LATE_OUT = 2
PARTS = 7
f32, bf16 = jnp.float32, jnp.bfloat16


def kernel(
    plane, count, block,
    itab_own, itab_in, ftab_in, tok_a, tok_b, gate_hbm, up_hbm, down_hbm,
    out_ref,
    w_gate, w_up, w_down, itab_v, ftab_v, itab, ftab, tok_all, sent_a, sent_b, got_a, got_b, x_a, x_b, part,
    half_in, full_in, back_a, back_b, home_a, home_b, mix, mix_half, mix_full, wide32, acc, hid,
    w_sem, tab_s, tab_r, tab_l, tok_s, tok_r, tfw_s, tfw_r, pa_s, pa_r, pb_s, pb_r, ag_s, ag_r, fw_s, fw_r,
    rh_s, rh_r, rf_s, rf_r, ba_s, ba_r, bb_s, bb_r, mh_s, mh_r, mf_s, mf_r,
):
    node, local = lax.axis_index("node"), lax.axis_index("local")
    ys = lax.axis_size("local") // SHARDS
    y, z = local // SHARDS, local % SHARDS
    me = node * ys + y
    nxt, far, prv = [(z + d) % SHARDS for d in (1, 2, 3)]
    nxt_dev, far_dev, prv_dev = [(node, y * SHARDS + q) for q in (nxt, far, prv)]
    z_devs = (nxt_dev, far_dev, prv_dev)
    hidden = w_gate.shape[1]
    step_subs = block // LANES
    in_a, in_b = (PARTS - LATE_IN) * step_subs, LATE_IN * step_subs
    out_a, out_b = (PARTS - LATE_OUT) * step_subs, LATE_OUT * step_subs
    half, half_t = plane // 2, count // 2
    rows = SHARDS * plane
    low, high = pl.ds(0, half), pl.ds(half, half)

    def loop(n, body, start=0, unroll=1):
        def wrapped(i, carry):
            body(i)
            return carry

        lax.fori_loop(start, n, wrapped, 0, unroll=unroll)

    w_copies = [
        pltpu.make_async_copy(gate_hbm.at[0], w_gate, w_sem.at[0]),
        pltpu.make_async_copy(up_hbm.at[0], w_up, w_sem.at[1]),
        pltpu.make_async_copy(down_hbm.at[0], w_down, w_sem.at[2]),
    ]
    for copy in w_copies:
        copy.start()

    def peer(k):
        other = lax.rem(me + k, plane)
        return other, (other // ys, (other % ys) * SHARDS + z)

    barrier = pltpu.get_barrier_semaphore()

    @functools.partial(loop, plane, start=1)
    def _(k):
        pl.semaphore_signal(barrier, inc=1, device_id=peer(k)[1], device_id_type=MESH)

    for dev in z_devs:
        pl.semaphore_signal(barrier, inc=1, device_id=dev, device_id_type=MESH)

    def remote(src, dst, s_sem, r_sem, dev):
        return pltpu.make_async_remote_copy(
            src_ref=src, dst_ref=dst, send_sem=s_sem, recv_sem=r_sem, device_id=dev, device_id_type=MESH
        )

    def spread(src, dst, s_sem, r_sem, c):
        @functools.partial(loop, plane, start=1)
        def _(k):
            other, dev = peer(k)
            remote(src.at[c, other], dst.at[c, me], s_sem.at[c], r_sem.at[c], dev).start()

        dst[c, me] = src[c, me]

    def spread_all(src, dst, s_sem, r_sem, c):
        some = pl.ds(0, plane - 1)
        return remote(src.at[c, some], dst.at[c, some], s_sem.at[c], r_sem.at[c], nxt_dev)

    plane_a = functools.partial(spread_all, sent_a, got_a, pa_s, pa_r)
    plane_b = functools.partial(spread_all, sent_b, got_b, pb_s, pb_r)
    return_a = functools.partial(spread_all, back_a, home_a, ba_s, ba_r)
    return_b = functools.partial(spread_all, back_b, home_b, bb_s, bb_r)

    def tables():
        copies = []
        for d, dev in enumerate(z_devs):
            copies.append(remote(itab_in, itab_v.at[z], tab_s.at[d, 0], tab_r.at[d, 0], dev))
            copies.append(remote(ftab_in, ftab_v.at[z], tab_s.at[d, 1], tab_r.at[d, 1], dev))
        return copies

    def gather_tokens():
        return (
            remote(tok_b, tok_all.at[z], tok_s.at[0], tok_r.at[0], nxt_dev),
            remote(tok_b, tok_all.at[z], tok_s.at[1], tok_r.at[1], prv_dev),
        )

    def forward_tokens():
        first, second = pl.ds(0, half_t), pl.ds(half_t, half_t)
        return (
            remote(tok_all.at[prv, first], tok_all.at[prv, first], tfw_s.at[0], tfw_r.at[0], nxt_dev),
            remote(tok_all.at[nxt, second], tok_all.at[nxt, second], tfw_s.at[1], tfw_r.at[1], prv_dev),
        )

    def gather(c):
        return (
            remote(x_a.at[c, z], x_a.at[c, z], ag_s.at[c, 0], ag_r.at[c, 0], nxt_dev),
            remote(x_a.at[c, z], x_a.at[c, z], ag_s.at[c, 1], ag_r.at[c, 1], prv_dev),
        )

    def forward(c):
        return (
            remote(x_a.at[c, prv, low], x_a.at[c, prv, low], fw_s.at[c, 0], fw_r.at[c, 0], nxt_dev),
            remote(x_a.at[c, nxt, high], x_a.at[c, nxt, high], fw_s.at[c, 1], fw_r.at[c, 1], prv_dev),
        )

    def scatter_half(c):
        return (
            remote(part.at[c, far, low], half_in.at[c, 0], rh_s.at[c, 0], rh_r.at[c, 0], nxt_dev),
            remote(part.at[c, far, high], half_in.at[c, 1], rh_s.at[c, 1], rh_r.at[c, 1], prv_dev),
        )

    def scatter_full(c):
        return (
            remote(part.at[c, nxt], full_in.at[c, 0], rf_s.at[c, 0], rf_r.at[c, 0], nxt_dev),
            remote(part.at[c, prv], full_in.at[c, 1], rf_s.at[c, 1], rf_r.at[c, 1], prv_dev),
        )

    def mix_halves():
        first, second = pl.ds(0, half_t), pl.ds(half_t, half_t)
        return (
            remote(mix.at[far, first], mix_half.at[0], mh_s.at[0], mh_r.at[0], nxt_dev),
            remote(mix.at[far, second], mix_half.at[1], mh_s.at[1], mh_r.at[1], prv_dev),
        )

    def mix_fulls():
        return (
            remote(mix.at[nxt], mix_full.at[0], mf_s.at[0], mf_r.at[0], nxt_dev),
            remote(mix.at[prv], mix_full.at[1], mf_s.at[1], mf_r.at[1], prv_dev),
        )

    def launch_a(c):
        @functools.partial(loop, plane)
        def _(e):
            sent_a[c, e] = tok_a[itab_own[c // 4, (c % 4) * plane + e]]

        spread(sent_a, got_a, pa_s, pa_r, c)

    def launch_b(c):
        @functools.partial(loop, plane)
        def _(e):
            for q in range(SHARDS):
                sent_b[c, e, q] = tok_all[q, itab[q, c // 4, (c % 4) * plane + e]]

        spread(sent_b, got_b, pb_s, pb_r, c)

    def stage_a(c):
        plane_a(c).wait_recv()

        @functools.partial(loop, plane)
        def _(s):
            wide32[pl.ds(pl.multiple_of(s * in_a, 8), in_a), :] = got_a[c, s].astype(f32)

        @functools.partial(loop, in_a)
        def _(j):
            cols = pl.ds(pl.multiple_of(j * LANES, LANES), LANES)
            for s0 in range(0, plane, 16):
                pair = [wide32[pl.ds((s0 + d) * in_a + j, 8, stride=in_a), :] for d in (0, 8)]
                x_a[c, z, pl.ds(s0, 16), cols] = jnp.concatenate(pair, axis=0).astype(bf16)

        for copy in gather(c):
            copy.start()

    def stage_b(c):
        for copy in gather(c):
            copy.wait_recv()
        for copy in forward(c):
            copy.start()

    def stage_c(c):
        plane_b(c).wait_recv()

        @functools.partial(loop, plane)
        def _(p):
            for q in range(SHARDS):
                wide32[pl.ds(pl.multiple_of((q * plane + p) * in_b, 8), in_b), :] = got_b[c, p, q].astype(f32)

        @functools.partial(loop, in_b)
        def _(j):
            cols = pl.ds(pl.multiple_of(j * LANES, LANES), LANES)
            for s0 in range(0, rows, 16):
                pair = [wide32[pl.ds((s0 + d) * in_b + j, 8, stride=in_b), :] for d in (0, 8)]
                x_b[pl.ds(s0, 16), cols] = jnp.concatenate(pair, axis=0).astype(bf16)

        acc[...] = jnp.zeros_like(acc)

        def contract(rows_k, span):
            acc[:, :hidden] += jnp.dot(rows_k, w_gate[span, :], preferred_element_type=f32)
            acc[:, hidden:] += jnp.dot(rows_k, w_up[span, :], preferred_element_type=f32)

        @functools.partial(loop, LATE_IN)
        def _(k):
            here = pl.ds(pl.multiple_of(k * block, LANES), block)
            contract(x_b[:, here], pl.ds(pl.multiple_of((PARTS - LATE_IN + k) * block, LANES), block))

        for copy in forward(c):
            copy.wait_recv()

        @functools.partial(loop, PARTS - LATE_IN)
        def _(k):
            here = pl.ds(pl.multiple_of(k * block, LANES), block)
            contract(x_a[c, :, :, here].reshape(rows, block), here)

        gate = acc[:, :hidden]
        hid[...] = (gate / (1.0 + jnp.exp(-gate)) * acc[:, hidden:]).astype(bf16)

        @functools.partial(loop, PARTS - LATE_OUT)
        def _(k):
            span = pl.ds(pl.multiple_of(k * block, LANES), block)
            value = jnp.dot(hid[...], w_down[:, span], preferred_element_type=f32)
            part[c, :, :, span] = value.astype(bf16).reshape(SHARDS, plane, block)

        for copy in scatter_half(c):
            copy.start()

        @functools.partial(loop, LATE_OUT)
        def _(k):
            span = pl.ds(pl.multiple_of((PARTS - LATE_OUT + k) * block, LANES), block)
            value = jnp.dot(hid[...], w_down[:, span], preferred_element_type=f32)
            for j in range(step_subs):
                for s0 in range(0, rows, 8):
                    wide32[pl.ds(s0 * out_b + k * step_subs + j, 8, stride=out_b), :] = (
                        value[s0:s0 + 8, j * LANES:(j + 1) * LANES]
                    )

        @functools.partial(loop, plane)
        def _(p):
            for q in range(SHARDS):
                span = pl.ds(pl.multiple_of((q * plane + p) * out_b, 8), out_b)
                back_b[c, p, q] = wide32[span, :].astype(bf16)

        spread(back_b, home_b, bb_s, bb_r, c)

    def stage_e(c):
        for copy in scatter_half(c):
            copy.wait_recv()
        for side, owner, span in ((0, nxt, low), (1, prv, high)):
            mine = part[c, owner, span].astype(f32)
            part[c, owner, span] = (mine + half_in[c, side].astype(f32)).astype(bf16)
        for copy in scatter_full(c):
            copy.start()

    def stage_f(c):
        for copy in scatter_full(c):
            copy.wait_recv()

        @functools.partial(loop, out_a)
        def _(j):
            cols = pl.ds(pl.multiple_of(j * LANES, LANES), LANES)
            for s0 in range(0, plane, 16):
                span = pl.ds(s0, 16)
                value = part[c, z, span, cols].astype(f32)
                value = value + full_in[c, 0, span, cols].astype(f32)
                value = value + full_in[c, 1, span, cols].astype(f32)
                for d in (0, 8):
                    wide32[pl.ds((s0 + d) * out_a + j, 8, stride=out_a), :] = value[d:d + 8]

        @functools.partial(loop, plane)
        def _(s):
            back_a[c, s] = wide32[pl.ds(pl.multiple_of(s * out_a, 8), out_a), :].astype(bf16)

        spread(back_a, home_a, ba_s, ba_r, c)

    def weighted(source, q, t, subs, pick):
        total = jnp.zeros((subs, LANES), f32)
        for k in range(2):
            spot = itab[q, 2, t * 2 + k]
            total = total + ftab[q, 0, t * 2 + k] * pick(source, spot // plane, spot % plane)
        return total

    def mix_one(q):
        @functools.partial(loop, count)
        def _(t):
            take = lambda ref, c, e: ref[c, e, q].astype(f32)
            mix[q, t] = weighted(home_b, q, t, out_b, take).astype(bf16)

    pl.semaphore_wait(barrier, plane + 2)
    for copy in gather_tokens():
        copy.start()
    for copy in tables():
        copy.start()
    tok_all[z] = tok_b[...]
    loop(3, launch_a)
    for copy in gather_tokens():
        copy.wait_recv()
    for copy in forward_tokens():
        copy.start()

    def ready():
        for copy in tables():
            copy.wait_recv()
        moves = [
            pltpu.make_async_copy(itab_in, itab.at[z], tab_l.at[0]),
            pltpu.make_async_copy(ftab_in, ftab.at[z], tab_l.at[1]),
        ]
        for d, q in enumerate((nxt, far, prv)):
            moves.append(pltpu.make_async_copy(itab_v.at[q], itab.at[q], tab_l.at[2 + 2 * d]))
            moves.append(pltpu.make_async_copy(ftab_v.at[q], ftab.at[q], tab_l.at[3 + 2 * d]))
        for move in moves:
            move.start()
        for move in moves:
            move.wait()
        for copy in forward_tokens():
            copy.wait_recv()
        for copy in w_copies:
            copy.wait()

    def late(c):
        launch_b(c)

        @pl.when(c + 3 < MOST)
        def _():
            launch_a(c + 3)

    stages = ((stage_a, 0), (late, 1), (stage_b, 1), (stage_c, 2), (stage_e, 3), (stage_f, 4))

    def run(s, skip_last=False):
        @pl.when(s == 1)
        def _():
            ready()

        for stage, lag in stages:
            c = s - lag

            @pl.when((c >= 0) & (c < MOST))
            def _(stage=stage, c=c):
                stage(c)

    loop(MOST + 3, run)

    @functools.partial(loop, MOST)
    def _(c):
        return_b(c).wait_recv()

    mix_one(far)
    for copy in mix_halves():
        copy.start()
    mix_one(nxt)
    mix_one(prv)
    mix_one(z)
    stage_f(MOST - 1)
    for copy in mix_halves():
        copy.wait_recv()
    for side, owner, start in ((0, nxt, 0), (1, prv, half_t)):
        @functools.partial(loop, half_t)
        def _(t):
            mix[owner, start + t] = (mix[owner, start + t].astype(f32) + mix_half[side, t].astype(f32)).astype(bf16)

    for copy in mix_fulls():
        copy.start()

    @functools.partial(loop, MOST)
    def _(c):
        return_a(c).wait_recv()

    @functools.partial(loop, count)
    def _(t):
        take = lambda ref, c, e: ref[c, e].astype(f32)
        out_ref[t, pl.ds(0, out_a)] = weighted(home_a, z, t, out_a, take).astype(bf16)

    for copy in mix_fulls():
        copy.wait_recv()

    @functools.partial(loop, count)
    def _(t):
        total = mix[z, t].astype(f32) + mix_full[0, t].astype(f32) + mix_full[1, t].astype(f32)
        out_ref[t, pl.ds(out_a, out_b)] = total.astype(bf16)

    for copy in (*tables(), *gather_tokens(), *forward_tokens(), *mix_halves(), *mix_fulls()):
        copy.wait_send()

    @functools.partial(loop, MOST)
    def _(c):
        for copy in (plane_a(c), plane_b(c), return_a(c), return_b(c)):
            copy.wait_send()
        for group in (gather, forward, scatter_half, scatter_full):
            for copy in group(c):
                copy.wait_send()


def per_device(tokens, routes, scores, gate_proj, up_proj, down_proj):
    plane = lax.axis_size("node") * (lax.axis_size("local") // SHARDS)
    count, wide = tokens.shape
    depth, hidden = gate_proj.shape[1:]
    block = wide // PARTS
    subs, step_subs = wide // LANES, block // LANES
    weights = (SCALE * scores / jnp.sum(scores, axis=1, keepdims=True)).astype(bf16).astype(f32)
    labels = jnp.arange(plane, dtype=jnp.int32)
    matches = routes[:, :, None] == labels[None, None, :]
    named = jnp.any(matches, axis=1)
    earlier = jnp.arange(count)[:, None] > jnp.arange(count)[None, :]
    rank = jnp.sum(earlier[:, :, None] & named[None], axis=1, dtype=jnp.int32)
    slots = jnp.arange(8, dtype=jnp.int32)
    chosen = named[None] & (rank[None] == slots[:, None, None]) & (slots < MOST)[:, None, None]
    pick = jnp.sum(jnp.where(chosen, jnp.arange(count, dtype=jnp.int32)[None, :, None], 0), axis=1)
    home = jnp.sum(jnp.where(matches, rank[:, None, :] * plane + labels[None, None, :], 0), axis=2)
    itab = jnp.zeros((8, LANES), jnp.int32)
    itab = itab.at[:2, :4 * plane].set(pick.reshape(2, 4 * plane)).at[2, :2 * count].set(home.reshape(-1))
    ftab = jnp.zeros((8, LANES), f32).at[0, :2 * count].set(weights.reshape(-1))
    in_a, in_b = (PARTS - LATE_IN) * step_subs, LATE_IN * step_subs
    out_a, out_b = (PARTS - LATE_OUT) * step_subs, LATE_OUT * step_subs
    tok = tokens.reshape(count, subs, LANES)
    dma = pltpu.SemaphoreType.DMA
    vmem, smem, hbm = pltpu.VMEM, pltpu.SMEM, pl.ANY
    sent_b = vmem((MOST, plane, SHARDS, in_b, LANES), bf16)
    out = pl.pallas_call(
        functools.partial(kernel, plane, count, block),
        out_shape=jax.ShapeDtypeStruct((count, subs, LANES), bf16),
        in_specs=[pl.BlockSpec(memory_space=m) for m in (smem, vmem, vmem, vmem, vmem, hbm, hbm, hbm)],
        out_specs=pl.BlockSpec(memory_space=vmem),
        scratch_shapes=[
            vmem((depth, hidden), bf16),
            vmem((depth, hidden), bf16),
            vmem((hidden, depth), bf16),
            vmem((SHARDS, 8, LANES), jnp.int32),
            vmem((SHARDS, 8, LANES), f32),
            smem((SHARDS, 8, LANES), jnp.int32),
            smem((SHARDS, 8, LANES), f32),
            vmem((SHARDS, count, in_b, LANES), bf16),
            vmem((MOST, plane, in_a, LANES), bf16),
            vmem((MOST, plane, SHARDS, in_b, LANES), bf16),
            vmem((MOST, plane, in_a, LANES), bf16),
            vmem((MOST, plane, SHARDS, in_b, LANES), bf16),
            vmem((MOST, SHARDS, plane, in_a * LANES), bf16),
            vmem((SHARDS * plane, in_b * LANES), bf16),
            vmem((MOST, SHARDS, plane, out_a * LANES), bf16),
            vmem((MOST, 2, plane // 2, out_a * LANES), bf16),
            vmem((MOST, 2, plane, out_a * LANES), bf16),
            vmem((MOST, plane, out_a, LANES), bf16),
            vmem((MOST, plane, SHARDS, out_b, LANES), bf16),
            vmem((MOST, plane, out_a, LANES), bf16),
            vmem((MOST, plane, SHARDS, out_b, LANES), bf16),
            vmem((SHARDS, count, out_b, LANES), bf16),
            vmem((2, count // 2, out_b, LANES), bf16),
            vmem((2, count, out_b, LANES), bf16),
            vmem((plane * max(in_a, out_a, SHARDS * in_b, SHARDS * out_b), LANES), f32),
            vmem((SHARDS * plane, 2 * hidden), f32),
            vmem((SHARDS * plane, hidden), bf16),
            dma((3,)),
            dma((3, 2)), dma((3, 2)), dma((8,)),
            dma((2,)), dma((2,)),
            dma((2,)), dma((2,)),
            dma((MOST,)), dma((MOST,)),
            dma((MOST,)), dma((MOST,)),
            dma((MOST, 2)), dma((MOST, 2)),
            dma((MOST, 2)), dma((MOST, 2)),
            dma((MOST, 2)), dma((MOST, 2)),
            dma((MOST, 2)), dma((MOST, 2)),
            dma((MOST,)), dma((MOST,)),
            dma((MOST,)), dma((MOST,)),
            dma((2,)), dma((2,)),
            dma((2,)), dma((2,)),
        ],
        compiler_params=pltpu.CompilerParams(
            collective_id=0, has_side_effects=True, vmem_limit_bytes=67043328
        ),
    )(itab, itab, ftab, tok[:, :in_a], tok[:, in_a:], gate_proj, up_proj, down_proj)
    return out.reshape(count, wide)


def solution(mesh):
    both = ("node", "local")
    return jax.shard_map(
        per_device,
        mesh=mesh,
        in_specs=(P(both, None),) * 3 + (P(both, None, None),) * 3,
        out_specs=P(both, None),
        check_vma=False,
    )
```

```python
import functools

import jax
import jax.numpy as jnp
from jax import lax
from jax.experimental import pallas as pl
from jax.experimental.pallas import tpu as pltpu
from jax.sharding import PartitionSpec as P

MESH = pl.DeviceIdType.MESH
SHARDS = 4
SCALE = 2.827
MOST = 5
LANES = 128
LATE_IN = 2
LATE_OUT = 3
PARTS = 7
f32, bf16 = jnp.float32, jnp.bfloat16


def kernel(
    plane, count, block,
    routes_ref, scores_ref, tok_ref, gate_hbm, up_hbm, down_hbm,
    out_ref,
    w_gate, w_up, w_down, itab_in, ftab_in, itab_v, ftab_v, itab, ftab, tok_all, tok_a, sent_a, sent_b, got_a, got_b, x_a, x_b, part,
    half_in, full_in, back_a, back_b, home_a, home_b, mix, mix_half, mix_full, wide32, acc, hid,
    w_sem, tab_s, tab_r, tab_l, tok_s, tok_r, tfw_s, tfw_r, pa_s, pa_r, pb_s, pb_r, ag_s, ag_r, fw_s, fw_r,
    rh_s, rh_r, rf_s, rf_r, ba_s, ba_r, bb_s, bb_r, mh_s, mh_r, mf_s, mf_r,
):
    node, local = lax.axis_index("node"), lax.axis_index("local")
    ys = lax.axis_size("local") // SHARDS
    y, z = local // SHARDS, local % SHARDS
    me = node * ys + y
    nxt, far, prv = [(z + d) % SHARDS for d in (1, 2, 3)]
    nxt_dev, far_dev, prv_dev = [(node, y * SHARDS + q) for q in (nxt, far, prv)]
    z_devs = (nxt_dev, far_dev, prv_dev)
    hidden = w_gate.shape[1]
    step_subs = block // LANES
    subs = PARTS * step_subs
    in_a, in_b = (PARTS - LATE_IN) * step_subs, LATE_IN * step_subs
    out_a, out_b = (PARTS - LATE_OUT) * step_subs, LATE_OUT * step_subs
    half, half_t = plane // 2, count // 2
    rows = SHARDS * plane
    low, high = pl.ds(0, half), pl.ds(half, half)

    def loop(n, body, start=0, unroll=1):
        def wrapped(i, carry):
            body(i)
            return carry

        lax.fori_loop(start, n, wrapped, 0, unroll=unroll)

    w_copies = [
        pltpu.make_async_copy(gate_hbm.at[0], w_gate, w_sem.at[0]),
        pltpu.make_async_copy(up_hbm.at[0], w_up, w_sem.at[1]),
        pltpu.make_async_copy(down_hbm.at[0], w_down, w_sem.at[2]),
    ]
    for copy in w_copies:
        copy.start()

    def peer(k):
        other = lax.rem(me + k, plane)
        return other, (other // ys, (other % ys) * SHARDS + z)

    barrier = pltpu.get_barrier_semaphore()

    @functools.partial(loop, plane, start=1)
    def _(k):
        pl.semaphore_signal(barrier, inc=1, device_id=peer(k)[1], device_id_type=MESH)

    for dev in z_devs:
        pl.semaphore_signal(barrier, inc=1, device_id=dev, device_id_type=MESH)

    def remote(src, dst, s_sem, r_sem, dev):
        return pltpu.make_async_remote_copy(
            src_ref=src, dst_ref=dst, send_sem=s_sem, recv_sem=r_sem, device_id=dev, device_id_type=MESH
        )

    def spread(src, dst, s_sem, r_sem, c):
        @functools.partial(loop, plane, start=1)
        def _(k):
            other, dev = peer(k)
            remote(src.at[c, other], dst.at[c, me], s_sem.at[c], r_sem.at[c], dev).start()

        dst[c, me] = src[c, me]

    def spread_all(src, dst, s_sem, r_sem, c):
        some = pl.ds(0, plane - 1)
        return remote(src.at[c, some], dst.at[c, some], s_sem.at[c], r_sem.at[c], nxt_dev)

    plane_a = functools.partial(spread_all, sent_a, got_a, pa_s, pa_r)
    plane_b = functools.partial(spread_all, sent_b, got_b, pb_s, pb_r)
    return_a = functools.partial(spread_all, back_a, home_a, ba_s, ba_r)
    return_b = functools.partial(spread_all, back_b, home_b, bb_s, bb_r)

    def tables():
        copies = []
        for d, dev in enumerate(z_devs):
            copies.append(remote(itab_in, itab_v.at[z], tab_s.at[d, 0], tab_r.at[d, 0], dev))
            copies.append(remote(ftab_in, ftab_v.at[z], tab_s.at[d, 1], tab_r.at[d, 1], dev))
        return copies

    def gather_tokens():
        return (
            remote(tok_all.at[z], tok_all.at[z], tok_s.at[0], tok_r.at[0], nxt_dev),
            remote(tok_all.at[z], tok_all.at[z], tok_s.at[1], tok_r.at[1], prv_dev),
        )

    def forward_tokens():
        first, second = pl.ds(0, half_t), pl.ds(half_t, half_t)
        return (
            remote(tok_all.at[prv, first], tok_all.at[prv, first], tfw_s.at[0], tfw_r.at[0], nxt_dev),
            remote(tok_all.at[nxt, second], tok_all.at[nxt, second], tfw_s.at[1], tfw_r.at[1], prv_dev),
        )

    def gather(c):
        return (
            remote(x_a.at[c, z], x_a.at[c, z], ag_s.at[c, 0], ag_r.at[c, 0], nxt_dev),
            remote(x_a.at[c, z], x_a.at[c, z], ag_s.at[c, 1], ag_r.at[c, 1], prv_dev),
        )

    def forward(c):
        return (
            remote(x_a.at[c, prv, low], x_a.at[c, prv, low], fw_s.at[c, 0], fw_r.at[c, 0], nxt_dev),
            remote(x_a.at[c, nxt, high], x_a.at[c, nxt, high], fw_s.at[c, 1], fw_r.at[c, 1], prv_dev),
        )

    def scatter_half(c):
        return (
            remote(part.at[c, far, low], half_in.at[c, 0], rh_s.at[c, 0], rh_r.at[c, 0], nxt_dev),
            remote(part.at[c, far, high], half_in.at[c, 1], rh_s.at[c, 1], rh_r.at[c, 1], prv_dev),
        )

    def scatter_full(c):
        return (
            remote(part.at[c, nxt], full_in.at[c, 0], rf_s.at[c, 0], rf_r.at[c, 0], nxt_dev),
            remote(part.at[c, prv], full_in.at[c, 1], rf_s.at[c, 1], rf_r.at[c, 1], prv_dev),
        )

    def mix_halves():
        first, second = pl.ds(0, half_t), pl.ds(half_t, half_t)
        return (
            remote(mix.at[far, first], mix_half.at[0], mh_s.at[0], mh_r.at[0], nxt_dev),
            remote(mix.at[far, second], mix_half.at[1], mh_s.at[1], mh_r.at[1], prv_dev),
        )

    def mix_fulls():
        return (
            remote(mix.at[nxt], mix_full.at[0], mf_s.at[0], mf_r.at[0], nxt_dev),
            remote(mix.at[prv], mix_full.at[1], mf_s.at[1], mf_r.at[1], prv_dev),
        )

    def fill_a(c):
        @functools.partial(loop, plane)
        def _(e):
            sent_a[c, e] = tok_a[itab[z, c // 4, (c % 4) * plane + e]]

    def launch_a(c):
        spread(sent_a, got_a, pa_s, pa_r, c)

    def launch_b(c):
        @functools.partial(loop, plane)
        def _(e):
            for q in range(SHARDS):
                sent_b[c, e, q] = tok_all[q, itab[q, c // 4, (c % 4) * plane + e]]

        spread(sent_b, got_b, pb_s, pb_r, c)

    def stage_a(c):
        plane_a(c).wait_recv()

        @functools.partial(loop, plane)
        def _(s):
            wide32[pl.ds(pl.multiple_of(s * in_a, 8), in_a), :] = got_a[c, s].astype(f32)

        @functools.partial(loop, in_a)
        def _(j):
            cols = pl.ds(pl.multiple_of(j * LANES, LANES), LANES)
            for s0 in range(0, plane, 16):
                pair = [wide32[pl.ds((s0 + d) * in_a + j, 8, stride=in_a), :] for d in (0, 8)]
                x_a[c, z, pl.ds(s0, 16), cols] = jnp.concatenate(pair, axis=0).astype(bf16)

        for copy in gather(c):
            copy.start()

    def stage_b(c):
        for copy in gather(c):
            copy.wait_recv()
        for copy in forward(c):
            copy.start()

    def stage_c(c):
        plane_b(c).wait_recv()

        @functools.partial(loop, plane)
        def _(p):
            for q in range(SHARDS):
                wide32[pl.ds(pl.multiple_of((q * plane + p) * in_b, 8), in_b), :] = got_b[c, p, q].astype(f32)

        @functools.partial(loop, in_b)
        def _(j):
            cols = pl.ds(pl.multiple_of(j * LANES, LANES), LANES)
            for s0 in range(0, rows, 16):
                pair = [wide32[pl.ds((s0 + d) * in_b + j, 8, stride=in_b), :] for d in (0, 8)]
                x_b[pl.ds(s0, 16), cols] = jnp.concatenate(pair, axis=0).astype(bf16)

        acc[...] = jnp.zeros_like(acc)

        def contract(rows_k, span):
            acc[:, :hidden] += jnp.dot(rows_k, w_gate[span, :], preferred_element_type=f32)
            acc[:, hidden:] += jnp.dot(rows_k, w_up[span, :], preferred_element_type=f32)

        @functools.partial(loop, LATE_IN)
        def _(k):
            here = pl.ds(pl.multiple_of(k * block, LANES), block)
            contract(x_b[:, here], pl.ds(pl.multiple_of((PARTS - LATE_IN + k) * block, LANES), block))

        for copy in forward(c):
            copy.wait_recv()

        @functools.partial(loop, PARTS - LATE_IN)
        def _(k):
            here = pl.ds(pl.multiple_of(k * block, LANES), block)
            contract(x_a[c, :, :, here].reshape(rows, block), here)

        gate = acc[:, :hidden]
        hid[...] = (gate / (1.0 + jnp.exp(-gate)) * acc[:, hidden:]).astype(bf16)

        @functools.partial(loop, PARTS - LATE_OUT)
        def _(k):
            span = pl.ds(pl.multiple_of(k * block, LANES), block)
            value = jnp.dot(hid[...], w_down[:, span], preferred_element_type=f32)
            part[c, :, :, span] = value.astype(bf16).reshape(SHARDS, plane, block)

        for copy in scatter_half(c):
            copy.start()

        @functools.partial(loop, LATE_OUT)
        def _(k):
            span = pl.ds(pl.multiple_of((PARTS - LATE_OUT + k) * block, LANES), block)
            value = jnp.dot(hid[...], w_down[:, span], preferred_element_type=f32)
            for j in range(step_subs):
                for s0 in range(0, rows, 8):
                    wide32[pl.ds(s0 * out_b + k * step_subs + j, 8, stride=out_b), :] = (
                        value[s0:s0 + 8, j * LANES:(j + 1) * LANES]
                    )

        @functools.partial(loop, plane)
        def _(p):
            for q in range(SHARDS):
                span = pl.ds(pl.multiple_of((q * plane + p) * out_b, 8), out_b)
                back_b[c, p, q] = wide32[span, :].astype(bf16)

        spread(back_b, home_b, bb_s, bb_r, c)

    def stage_e(c):
        for copy in scatter_half(c):
            copy.wait_recv()
        for side, owner, span in ((0, nxt, low), (1, prv, high)):
            mine = part[c, owner, span].astype(f32)
            part[c, owner, span] = (mine + half_in[c, side].astype(f32)).astype(bf16)
        for copy in scatter_full(c):
            copy.start()

    def stage_f(c):
        for copy in scatter_full(c):
            copy.wait_recv()

        @functools.partial(loop, out_a)
        def _(j):
            cols = pl.ds(pl.multiple_of(j * LANES, LANES), LANES)
            for s0 in range(0, plane, 16):
                span = pl.ds(s0, 16)
                value = part[c, z, span, cols].astype(f32)
                value = value + full_in[c, 0, span, cols].astype(f32)
                value = value + full_in[c, 1, span, cols].astype(f32)
                for d in (0, 8):
                    wide32[pl.ds((s0 + d) * out_a + j, 8, stride=out_a), :] = value[d:d + 8]

        @functools.partial(loop, plane)
        def _(s):
            back_a[c, s] = wide32[pl.ds(pl.multiple_of(s * out_a, 8), out_a), :].astype(bf16)

        spread(back_a, home_a, ba_s, ba_r, c)

    def weighted(source, q, t, subs, pick):
        total = jnp.zeros((subs, LANES), f32)
        for k in range(2):
            spot = itab[q, 2 + k, t]
            total = total + ftab[q, k, t] * pick(source, spot // plane, spot % plane)
        return total

    def mix_one(q):
        @functools.partial(loop, count)
        def _(t):
            take = lambda ref, c, e: ref[c, e, q].astype(f32)
            mix[q, t] = weighted(home_b, q, t, out_b, take).astype(bf16)

    def own_tables():
        routes, scores = routes_ref[...], scores_ref[...]
        expert = lax.broadcasted_iota(jnp.int32, (plane, count), 0)
        firsts, seconds = expert == routes[0:1, :], expert == routes[1:2, :]
        named = jnp.where(firsts | seconds, 1, 0)
        token = lax.broadcasted_iota(jnp.int32, (plane, count), 1)
        rank = jnp.zeros((plane, count), jnp.int32)
        for t in range(count - 1):
            rank = rank + jnp.where(token > t, named[:, t:t + 1], 0)
        spot = jnp.minimum(rank, MOST - 1) * plane + expert
        itab_in[...] = jnp.zeros_like(itab_in)
        ftab_in[...] = jnp.zeros_like(ftab_in)
        lane = lax.broadcasted_iota(jnp.int32, (plane, LANES), 1)
        sub = lax.broadcasted_iota(jnp.int32, (plane, LANES), 0)
        for row, slots in ((0, range(4)), (1, range(4, MOST))):
            spread_out = jnp.zeros((plane, LANES), jnp.int32)
            for c in slots:
                pick = jnp.sum(jnp.where(rank == c, named * token, 0), axis=1, keepdims=True)
                spread_out = spread_out + jnp.where(lane == sub + (c % 4) * plane, pick, 0)
            itab_in[row:row + 1, :] = jnp.sum(spread_out, axis=0, keepdims=True)
        weights = (SCALE * scores / (scores[0:1, :] + scores[1:2, :])).astype(bf16).astype(f32)
        for k, match in enumerate((firsts, seconds)):
            where = jnp.sum(jnp.where(match, spot, 0), axis=0, keepdims=True)
            itab_in[2 + k:3 + k, 0:count] = where
            ftab_in[k:k + 1, 0:count] = weights[k:k + 1, :]

    own_tables()

    @functools.partial(loop, subs)
    def _(j):
        cols = pl.ds(pl.multiple_of(j * LANES, LANES), LANES)
        for t0 in range(0, count, 16):
            value = tok_ref[pl.ds(t0, 16), cols].astype(f32)
            for d in (0, 8):
                wide32[pl.ds((t0 + d) * subs + j, 8, stride=subs), :] = value[d:d + 8]

    own_moves = [
        pltpu.make_async_copy(itab_in, itab.at[z], tab_l.at[0]),
        pltpu.make_async_copy(ftab_in, ftab.at[z], tab_l.at[1]),
    ]
    for move in own_moves:
        move.start()

    @functools.partial(loop, count)
    def _(t):
        tok_all[z, t] = wide32[pl.ds(pl.multiple_of(t * subs + in_a, 8), in_b), :].astype(bf16)
        tok_a[t] = wide32[pl.ds(pl.multiple_of(t * subs, 8), in_a), :].astype(bf16)

    for move in own_moves:
        move.wait()
    fill_a(0)
    pl.semaphore_wait(barrier, plane + 2)
    for copy in gather_tokens():
        copy.start()
    for copy in tables():
        copy.start()
    launch_a(0)
    for c in range(1, MOST):
        fill_a(c)
        if c < 3:
            launch_a(c)
    for copy in gather_tokens():
        copy.wait_recv()
    for copy in forward_tokens():
        copy.start()

    def ready():
        for copy in tables():
            copy.wait_recv()
        moves = []
        for d, q in enumerate((nxt, far, prv)):
            moves.append(pltpu.make_async_copy(itab_v.at[q], itab.at[q], tab_l.at[2 + 2 * d]))
            moves.append(pltpu.make_async_copy(ftab_v.at[q], ftab.at[q], tab_l.at[3 + 2 * d]))
        for move in moves:
            move.start()
        for move in moves:
            move.wait()
        for copy in forward_tokens():
            copy.wait_recv()
        for copy in w_copies:
            copy.wait()

    def late(c):
        launch_b(c)

        @pl.when(c + 3 < MOST)
        def _():
            launch_a(c + 3)

    stages = ((stage_a, 0), (late, 1), (stage_b, 1), (stage_c, 2), (stage_e, 3), (stage_f, 4))

    def run(s, skip_last=False):
        @pl.when(s == 1)
        def _():
            ready()

        for stage, lag in stages:
            c = s - lag

            @pl.when((c >= 0) & (c < MOST))
            def _(stage=stage, c=c):
                stage(c)

    loop(MOST + 3, run)

    @functools.partial(loop, MOST)
    def _(c):
        return_b(c).wait_recv()

    mix_one(far)
    for copy in mix_halves():
        copy.start()
    mix_one(nxt)
    mix_one(prv)
    mix_one(z)
    stage_f(MOST - 1)
    for copy in mix_halves():
        copy.wait_recv()
    for side, owner, start in ((0, nxt, 0), (1, prv, half_t)):
        @functools.partial(loop, half_t)
        def _(t):
            mix[owner, start + t] = (mix[owner, start + t].astype(f32) + mix_half[side, t].astype(f32)).astype(bf16)

    for copy in mix_fulls():
        copy.start()

    @functools.partial(loop, MOST)
    def _(c):
        return_a(c).wait_recv()

    @functools.partial(loop, count)
    def _(t):
        take = lambda ref, c, e: ref[c, e].astype(f32)
        wide32[pl.ds(pl.multiple_of(t * subs, 8), out_a), :] = weighted(home_a, z, t, out_a, take)

    def settle(j):
        cols = pl.ds(pl.multiple_of(j * LANES, LANES), LANES)
        for t0 in range(0, count, 16):
            pair = [wide32[pl.ds((t0 + d) * subs + j, 8, stride=subs), :] for d in (0, 8)]
            out_ref[pl.ds(t0, 16), cols] = jnp.concatenate(pair, axis=0).astype(bf16)

    loop(out_a, settle)
    for copy in mix_fulls():
        copy.wait_recv()

    @functools.partial(loop, count)
    def _(t):
        total = mix[z, t].astype(f32) + mix_full[0, t].astype(f32) + mix_full[1, t].astype(f32)
        wide32[pl.ds(pl.multiple_of(t * subs + out_a, 8), out_b), :] = total

    loop(subs, settle, start=out_a)
    for copy in (*tables(), *gather_tokens(), *forward_tokens(), *mix_halves(), *mix_fulls()):
        copy.wait_send()

    @functools.partial(loop, MOST)
    def _(c):
        for copy in (plane_a(c), plane_b(c), return_a(c), return_b(c)):
            copy.wait_send()
        for group in (gather, forward, scatter_half, scatter_full):
            for copy in group(c):
                copy.wait_send()


def per_device(tokens, routes, scores, gate_proj, up_proj, down_proj):
    plane = lax.axis_size("node") * (lax.axis_size("local") // SHARDS)
    count, wide = tokens.shape
    depth, hidden = gate_proj.shape[1:]
    block = wide // PARTS
    subs, step_subs = wide // LANES, block // LANES
    in_a, in_b = (PARTS - LATE_IN) * step_subs, LATE_IN * step_subs
    out_a, out_b = (PARTS - LATE_OUT) * step_subs, LATE_OUT * step_subs
    dma = pltpu.SemaphoreType.DMA
    vmem, smem, hbm = pltpu.VMEM, pltpu.SMEM, pl.ANY
    return pl.pallas_call(
        functools.partial(kernel, plane, count, block),
        out_shape=jax.ShapeDtypeStruct((count, wide), bf16),
        in_specs=[pl.BlockSpec(memory_space=m) for m in (vmem, vmem, vmem, hbm, hbm, hbm)],
        out_specs=pl.BlockSpec(memory_space=vmem),
        scratch_shapes=[
            vmem((depth, hidden), bf16),
            vmem((depth, hidden), bf16),
            vmem((hidden, depth), bf16),
            vmem((8, LANES), jnp.int32),
            vmem((8, LANES), f32),
            vmem((SHARDS, 8, LANES), jnp.int32),
            vmem((SHARDS, 8, LANES), f32),
            smem((SHARDS, 8, LANES), jnp.int32),
            smem((SHARDS, 8, LANES), f32),
            vmem((SHARDS, count, in_b, LANES), bf16),
            vmem((count, in_a, LANES), bf16),
            vmem((MOST, plane, in_a, LANES), bf16),
            vmem((MOST, plane, SHARDS, in_b, LANES), bf16),
            vmem((MOST, plane, in_a, LANES), bf16),
            vmem((MOST, plane, SHARDS, in_b, LANES), bf16),
            vmem((MOST, SHARDS, plane, in_a * LANES), bf16),
            vmem((SHARDS * plane, in_b * LANES), bf16),
            vmem((MOST, SHARDS, plane, out_a * LANES), bf16),
            vmem((MOST, 2, plane // 2, out_a * LANES), bf16),
            vmem((MOST, 2, plane, out_a * LANES), bf16),
            vmem((MOST, plane, out_a, LANES), bf16),
            vmem((MOST, plane, SHARDS, out_b, LANES), bf16),
            vmem((MOST, plane, out_a, LANES), bf16),
            vmem((MOST, plane, SHARDS, out_b, LANES), bf16),
            vmem((SHARDS, count, out_b, LANES), bf16),
            vmem((2, count // 2, out_b, LANES), bf16),
            vmem((2, count, out_b, LANES), bf16),
            vmem((max(plane * max(in_a, out_a, SHARDS * in_b, SHARDS * out_b), count * subs), LANES), f32),
            vmem((SHARDS * plane, 2 * hidden), f32),
            vmem((SHARDS * plane, hidden), bf16),
            dma((3,)),
            dma((3, 2)), dma((3, 2)), dma((8,)),
            dma((2,)), dma((2,)),
            dma((2,)), dma((2,)),
            dma((MOST,)), dma((MOST,)),
            dma((MOST,)), dma((MOST,)),
            dma((MOST, 2)), dma((MOST, 2)),
            dma((MOST, 2)), dma((MOST, 2)),
            dma((MOST, 2)), dma((MOST, 2)),
            dma((MOST, 2)), dma((MOST, 2)),
            dma((MOST,)), dma((MOST,)),
            dma((MOST,)), dma((MOST,)),
            dma((2,)), dma((2,)),
            dma((2,)), dma((2,)),
        ],
        compiler_params=pltpu.CompilerParams(
            collective_id=0, has_side_effects=True, vmem_limit_bytes=67043328
        ),
    )(routes.T, scores.T, tokens, gate_proj, up_proj, down_proj)


def solution(mesh):
    both = ("node", "local")
    return jax.shard_map(
        per_device,
        mesh=mesh,
        in_specs=(P(both, None),) * 3 + (P(both, None, None),) * 3,
        out_specs=P(both, None),
        check_vma=False,
    )
```

```python
import functools

import jax
import jax.numpy as jnp
from jax import lax
from jax.experimental import pallas as pl
from jax.experimental.pallas import tpu as pltpu
from jax.sharding import PartitionSpec as P

MESH = pl.DeviceIdType.MESH
SHARDS = 4
SCALE = 2.827
MOST = 5
LANES = 128
LATE_IN = 2
LATE_OUT = 3
PARTS = 7
UNROLL = 4
f32, bf16 = jnp.float32, jnp.bfloat16


def kernel(
    plane, count, block,
    routes_ref, scores_ref, tok_ref, gate_hbm, up_hbm, down_hbm,
    out_ref,
    w_gate, w_up, w_down, itab_in, ftab_in, itab_v, ftab_v, itab, ftab, tok_all, tok_a, sent_a, sent_b, got_a, got_b, x_a, x_b, part,
    half_in, full_in, back_a, back_b, home_a, home_b, mix, mix_half, mix_full, wide32, acc, hid,
    w_sem, tab_s, tab_r, tab_l, tok_s, tok_r, tfw_s, tfw_r, pa_s, pa_r, pb_s, pb_r, ag_s, ag_r, fw_s, fw_r,
    rh_s, rh_r, rf_s, rf_r, ba_s, ba_r, bb_s, bb_r, mh_s, mh_r, mf_s, mf_r,
):
    node, local = lax.axis_index("node"), lax.axis_index("local")
    ys = lax.axis_size("local") // SHARDS
    y, z = local // SHARDS, local % SHARDS
    me = node * ys + y
    nxt, far, prv = [(z + d) % SHARDS for d in (1, 2, 3)]
    nxt_dev, far_dev, prv_dev = [(node, y * SHARDS + q) for q in (nxt, far, prv)]
    z_devs = (nxt_dev, far_dev, prv_dev)
    hidden = w_gate.shape[1]
    step_subs = block // LANES
    subs = PARTS * step_subs
    in_a, in_b = (PARTS - LATE_IN) * step_subs, LATE_IN * step_subs
    out_a, out_b = (PARTS - LATE_OUT) * step_subs, LATE_OUT * step_subs
    half, half_t = plane // 2, count // 2
    rows = SHARDS * plane
    low, high = pl.ds(0, half), pl.ds(half, half)

    def loop(n, body, start=0, unroll=UNROLL):
        def wrapped(i, carry):
            body(i)
            return carry

        lax.fori_loop(start, n, wrapped, 0, unroll=unroll)

    w_copies = [
        pltpu.make_async_copy(gate_hbm.at[0], w_gate, w_sem.at[0]),
        pltpu.make_async_copy(up_hbm.at[0], w_up, w_sem.at[1]),
        pltpu.make_async_copy(down_hbm.at[0], w_down, w_sem.at[2]),
    ]
    for copy in w_copies:
        copy.start()

    def peer(k):
        other = lax.rem(me + k, plane)
        return other, (other // ys, (other % ys) * SHARDS + z)

    barrier = pltpu.get_barrier_semaphore()

    @functools.partial(loop, plane, start=1, unroll=plane - 1)
    def _(k):
        pl.semaphore_signal(barrier, inc=1, device_id=peer(k)[1], device_id_type=MESH)

    for dev in z_devs:
        pl.semaphore_signal(barrier, inc=1, device_id=dev, device_id_type=MESH)

    def remote(src, dst, s_sem, r_sem, dev):
        return pltpu.make_async_remote_copy(
            src_ref=src, dst_ref=dst, send_sem=s_sem, recv_sem=r_sem, device_id=dev, device_id_type=MESH
        )

    def spread(src, dst, s_sem, r_sem, c):
        @functools.partial(loop, plane, start=1, unroll=plane - 1)
        def _(k):
            other, dev = peer(k)
            remote(src.at[c, other], dst.at[c, me], s_sem.at[c], r_sem.at[c], dev).start()

        dst[c, me] = src[c, me]

    def spread_all(src, dst, s_sem, r_sem, c):
        some = pl.ds(0, plane - 1)
        return remote(src.at[c, some], dst.at[c, some], s_sem.at[c], r_sem.at[c], nxt_dev)

    plane_a = functools.partial(spread_all, sent_a, got_a, pa_s, pa_r)
    plane_b = functools.partial(spread_all, sent_b, got_b, pb_s, pb_r)
    return_a = functools.partial(spread_all, back_a, home_a, ba_s, ba_r)
    return_b = functools.partial(spread_all, back_b, home_b, bb_s, bb_r)

    def tables():
        copies = []
        for d, dev in enumerate(z_devs):
            copies.append(remote(itab_in, itab_v.at[z], tab_s.at[d, 0], tab_r.at[d, 0], dev))
            copies.append(remote(ftab_in, ftab_v.at[z], tab_s.at[d, 1], tab_r.at[d, 1], dev))
        return copies

    def both_ways(src_up, dst_up, src_dn, dst_dn, s_sem, r_sem):
        return (
            remote(src_up, dst_up, s_sem.at[0], r_sem.at[0], nxt_dev),
            remote(src_dn, dst_dn, s_sem.at[1], r_sem.at[1], prv_dev),
        )

    def same(ref_up, ref_dn, s_sem, r_sem):
        return both_ways(ref_up, ref_up, ref_dn, ref_dn, s_sem, r_sem)

    first, second = pl.ds(0, half_t), pl.ds(half_t, half_t)

    def lead_tokens():
        return same(tok_all.at[z, first], tok_all.at[z, second], tok_s.at[0], tok_r.at[0])

    def rest_tokens():
        return same(tok_all.at[z, second], tok_all.at[z, first], tok_s.at[1], tok_r.at[1])

    def forward_tokens():
        return same(tok_all.at[prv, first], tok_all.at[nxt, second], tfw_s, tfw_r)

    def lead(c):
        return same(x_a.at[c, z, low], x_a.at[c, z, high], ag_s.at[c, 0], ag_r.at[c, 0])

    def rest(c):
        return same(x_a.at[c, z, high], x_a.at[c, z, low], ag_s.at[c, 1], ag_r.at[c, 1])

    def forward(c):
        return same(x_a.at[c, prv, low], x_a.at[c, nxt, high], fw_s.at[c], fw_r.at[c])

    def scatter_far(c):
        return both_ways(
            part.at[c, far, low], half_in.at[c, 0], part.at[c, far, high], half_in.at[c, 1], rh_s.at[c], rh_r.at[c]
        )

    def scatter_pure(c):
        return both_ways(
            part.at[c, nxt, high], full_in.at[c, 0, high], part.at[c, prv, low], full_in.at[c, 1, low],
            rf_s.at[c, 0], rf_r.at[c, 0],
        )

    def scatter_sum(c):
        return both_ways(
            part.at[c, nxt, low], full_in.at[c, 0, low], part.at[c, prv, high], full_in.at[c, 1, high],
            rf_s.at[c, 1], rf_r.at[c, 1],
        )

    def mix_far():
        return both_ways(mix.at[far, first], mix_half.at[0], mix.at[far, second], mix_half.at[1], mh_s, mh_r)

    def mix_pure():
        return both_ways(
            mix.at[nxt, second], mix_full.at[0, second], mix.at[prv, first], mix_full.at[1, first],
            mf_s.at[0], mf_r.at[0],
        )

    def mix_sum():
        return both_ways(
            mix.at[nxt, first], mix_full.at[0, first], mix.at[prv, second], mix_full.at[1, second],
            mf_s.at[1], mf_r.at[1],
        )

    def start(*groups):
        for group in groups:
            for copy in group:
                copy.start()

    def await_in(*groups):
        for group in groups:
            for copy in group:
                copy.wait_recv()

    def fill_a(c):
        @functools.partial(loop, plane)
        def _(e):
            sent_a[c, e] = tok_a[itab[z, c // 4, (c % 4) * plane + e]]

    def launch_a(c):
        spread(sent_a, got_a, pa_s, pa_r, c)

    def launch_b(c):
        @functools.partial(loop, plane)
        def _(e):
            for q in range(SHARDS):
                sent_b[c, e, q] = tok_all[q, itab[q, c // 4, (c % 4) * plane + e]]

        spread(sent_b, got_b, pb_s, pb_r, c)

    def stage_a(c):
        plane_a(c).wait_recv()

        @functools.partial(loop, plane)
        def _(s):
            wide32[pl.ds(pl.multiple_of(s * in_a, 8), in_a), :] = got_a[c, s].astype(f32)

        @functools.partial(loop, in_a)
        def _(j):
            cols = pl.ds(pl.multiple_of(j * LANES, LANES), LANES)
            for s0 in range(0, plane, 16):
                pair = [wide32[pl.ds((s0 + d) * in_a + j, 8, stride=in_a), :] for d in (0, 8)]
                x_a[c, z, pl.ds(s0, 16), cols] = jnp.concatenate(pair, axis=0).astype(bf16)

        start(lead(c), rest(c))

    def stage_b(c):
        await_in(lead(c))
        start(forward(c))

    def stage_c(c):
        plane_b(c).wait_recv()

        @functools.partial(loop, plane)
        def _(p):
            for q in range(SHARDS):
                wide32[pl.ds(pl.multiple_of((q * plane + p) * in_b, 8), in_b), :] = got_b[c, p, q].astype(f32)

        @functools.partial(loop, in_b)
        def _(j):
            cols = pl.ds(pl.multiple_of(j * LANES, LANES), LANES)
            for s0 in range(0, rows, 16):
                pair = [wide32[pl.ds((s0 + d) * in_b + j, 8, stride=in_b), :] for d in (0, 8)]
                x_b[pl.ds(s0, 16), cols] = jnp.concatenate(pair, axis=0).astype(bf16)

        acc[...] = jnp.zeros_like(acc)

        def contract(rows_k, span):
            acc[:, :hidden] += jnp.dot(rows_k, w_gate[span, :], preferred_element_type=f32)
            acc[:, hidden:] += jnp.dot(rows_k, w_up[span, :], preferred_element_type=f32)

        @functools.partial(loop, LATE_IN, unroll=1)
        def _(k):
            here = pl.ds(pl.multiple_of(k * block, LANES), block)
            contract(x_b[:, here], pl.ds(pl.multiple_of((PARTS - LATE_IN + k) * block, LANES), block))

        await_in(rest(c), forward(c))

        @functools.partial(loop, PARTS - LATE_IN, unroll=1)
        def _(k):
            here = pl.ds(pl.multiple_of(k * block, LANES), block)
            contract(x_a[c, :, :, here].reshape(rows, block), here)

        gate = acc[:, :hidden]
        hid[...] = (gate / (1.0 + jnp.exp(-gate)) * acc[:, hidden:]).astype(bf16)

        @functools.partial(loop, LATE_OUT, unroll=1)
        def _(k):
            span = pl.ds(pl.multiple_of((PARTS - LATE_OUT + k) * block, LANES), block)
            value = jnp.dot(hid[...], w_down[:, span], preferred_element_type=f32)
            for j in range(step_subs):
                for s0 in range(0, rows, 8):
                    wide32[pl.ds(s0 * out_b + k * step_subs + j, 8, stride=out_b), :] = (
                        value[s0:s0 + 8, j * LANES:(j + 1) * LANES]
                    )

        @functools.partial(loop, plane)
        def _(p):
            for q in range(SHARDS):
                span = pl.ds(pl.multiple_of((q * plane + p) * out_b, 8), out_b)
                back_b[c, p, q] = wide32[span, :].astype(bf16)

        spread(back_b, home_b, bb_s, bb_r, c)

        @functools.partial(loop, PARTS - LATE_OUT, unroll=1)
        def _(k):
            span = pl.ds(pl.multiple_of(k * block, LANES), block)
            value = jnp.dot(hid[...], w_down[:, span], preferred_element_type=f32)
            part[c, :, :, span] = value.astype(bf16).reshape(SHARDS, plane, block)

        start(scatter_far(c), scatter_pure(c))

    def stage_e(c):
        await_in(scatter_far(c))
        for side, owner, span in ((0, nxt, low), (1, prv, high)):
            mine = part[c, owner, span].astype(f32)
            part[c, owner, span] = (mine + half_in[c, side].astype(f32)).astype(bf16)
        start(scatter_sum(c))

    def stage_f(c):
        await_in(scatter_pure(c), scatter_sum(c))

        @functools.partial(loop, out_a)
        def _(j):
            cols = pl.ds(pl.multiple_of(j * LANES, LANES), LANES)
            for s0 in range(0, plane, 16):
                span = pl.ds(s0, 16)
                value = part[c, z, span, cols].astype(f32)
                value = value + full_in[c, 0, span, cols].astype(f32)
                value = value + full_in[c, 1, span, cols].astype(f32)
                for d in (0, 8):
                    wide32[pl.ds((s0 + d) * out_a + j, 8, stride=out_a), :] = value[d:d + 8]

        @functools.partial(loop, plane)
        def _(s):
            back_a[c, s] = wide32[pl.ds(pl.multiple_of(s * out_a, 8), out_a), :].astype(bf16)

        spread(back_a, home_a, ba_s, ba_r, c)

    def weighted(source, q, t, subs, pick):
        total = jnp.zeros((subs, LANES), f32)
        for k in range(2):
            spot = itab[q, 2 + k, t]
            total = total + ftab[q, k, t] * pick(source, spot // plane, spot % plane)
        return total

    def mix_one(q):
        @functools.partial(loop, count)
        def _(t):
            take = lambda ref, c, e: ref[c, e, q].astype(f32)
            mix[q, t] = weighted(home_b, q, t, out_b, take).astype(bf16)

    def own_tables():
        routes, scores = routes_ref[...], scores_ref[...]
        expert = lax.broadcasted_iota(jnp.int32, (plane, count), 0)
        firsts, seconds = expert == routes[0:1, :], expert == routes[1:2, :]
        named = jnp.where(firsts | seconds, 1, 0)
        token = lax.broadcasted_iota(jnp.int32, (plane, count), 1)
        rank = jnp.zeros((plane, count), jnp.int32)
        for t in range(count - 1):
            rank = rank + jnp.where(token > t, named[:, t:t + 1], 0)
        spot = jnp.minimum(rank, MOST - 1) * plane + expert
        itab_in[...] = jnp.zeros_like(itab_in)
        ftab_in[...] = jnp.zeros_like(ftab_in)
        lane = lax.broadcasted_iota(jnp.int32, (plane, LANES), 1)
        sub = lax.broadcasted_iota(jnp.int32, (plane, LANES), 0)
        for row, slots in ((0, range(4)), (1, range(4, MOST))):
            spread_out = jnp.zeros((plane, LANES), jnp.int32)
            for c in slots:
                pick = jnp.sum(jnp.where(rank == c, named * token, 0), axis=1, keepdims=True)
                spread_out = spread_out + jnp.where(lane == sub + (c % 4) * plane, pick, 0)
            itab_in[row:row + 1, :] = jnp.sum(spread_out, axis=0, keepdims=True)
        weights = (SCALE * scores / (scores[0:1, :] + scores[1:2, :])).astype(bf16).astype(f32)
        for k, match in enumerate((firsts, seconds)):
            where = jnp.sum(jnp.where(match, spot, 0), axis=0, keepdims=True)
            itab_in[2 + k:3 + k, 0:count] = where
            ftab_in[k:k + 1, 0:count] = weights[k:k + 1, :]

    def unpack(j):
        cols = pl.ds(pl.multiple_of(j * LANES, LANES), LANES)
        for t0 in range(0, count, 16):
            value = tok_ref[pl.ds(t0, 16), cols].astype(f32)
            for d in (0, 8):
                wide32[pl.ds((t0 + d) * subs + j, 8, stride=subs), :] = value[d:d + 8]

    loop(subs, unpack, start=in_a)

    @functools.partial(loop, count)
    def _(t):
        tok_all[z, t] = wide32[pl.ds(pl.multiple_of(t * subs + in_a, 8), in_b), :].astype(bf16)

    own_tables()
    pl.semaphore_wait(barrier, plane + 2)
    start(lead_tokens(), rest_tokens())
    own_moves = [
        pltpu.make_async_copy(itab_in, itab.at[z], tab_l.at[0]),
        pltpu.make_async_copy(ftab_in, ftab.at[z], tab_l.at[1]),
    ]
    for move in own_moves:
        move.start()
    loop(in_a, unpack)

    @functools.partial(loop, count)
    def _(t):
        tok_a[t] = wide32[pl.ds(pl.multiple_of(t * subs, 8), in_a), :].astype(bf16)

    for move in own_moves:
        move.wait()
    fill_a(0)
    for copy in tables():
        copy.start()
    launch_a(0)
    for c in range(1, MOST):
        fill_a(c)
        if c < 3:
            launch_a(c)
    await_in(lead_tokens())
    start(forward_tokens())

    def ready():
        for copy in tables():
            copy.wait_recv()
        moves = []
        for d, q in enumerate((nxt, far, prv)):
            moves.append(pltpu.make_async_copy(itab_v.at[q], itab.at[q], tab_l.at[2 + 2 * d]))
            moves.append(pltpu.make_async_copy(ftab_v.at[q], ftab.at[q], tab_l.at[3 + 2 * d]))
        for move in moves:
            move.start()
        for move in moves:
            move.wait()
        await_in(rest_tokens(), forward_tokens())
        for copy in w_copies:
            copy.wait()

    def late(c):
        launch_b(c)

        @pl.when(c + 3 < MOST)
        def _():
            launch_a(c + 3)

    stages = ((stage_a, 0), (late, 1), (stage_b, 1), (stage_c, 2), (stage_e, 3), (stage_f, 4))

    def run(s, skip_last=False):
        @pl.when(s == 1)
        def _():
            ready()

        for stage, lag in stages:
            c = s - lag

            @pl.when((c >= 0) & (c < MOST))
            def _(stage=stage, c=c):
                stage(c)

    loop(MOST + 2, run, unroll=1)
    stage_e(MOST - 1)

    @functools.partial(loop, MOST, unroll=1)
    def _(c):
        return_b(c).wait_recv()

    mix_one(far)
    start(mix_far())
    mix_one(nxt)
    mix_one(prv)
    start(mix_pure())
    stage_f(MOST - 2)
    mix_one(z)
    await_in(mix_far())
    for side, owner, begin in ((0, nxt, 0), (1, prv, half_t)):
        @functools.partial(loop, half_t)
        def _(t):
            mix[owner, begin + t] = (mix[owner, begin + t].astype(f32) + mix_half[side, t].astype(f32)).astype(bf16)

    start(mix_sum())
    stage_f(MOST - 1)

    @functools.partial(loop, MOST, unroll=1)
    def _(c):
        return_a(c).wait_recv()

    @functools.partial(loop, count)
    def _(t):
        take = lambda ref, c, e: ref[c, e].astype(f32)
        wide32[pl.ds(pl.multiple_of(t * subs, 8), out_a), :] = weighted(home_a, z, t, out_a, take)

    def settle(j):
        cols = pl.ds(pl.multiple_of(j * LANES, LANES), LANES)
        for t0 in range(0, count, 16):
            pair = [wide32[pl.ds((t0 + d) * subs + j, 8, stride=subs), :] for d in (0, 8)]
            out_ref[pl.ds(t0, 16), cols] = jnp.concatenate(pair, axis=0).astype(bf16)

    loop(out_a, settle)
    await_in(mix_pure(), mix_sum())

    @functools.partial(loop, count)
    def _(t):
        total = mix[z, t].astype(f32) + mix_full[0, t].astype(f32) + mix_full[1, t].astype(f32)
        wide32[pl.ds(pl.multiple_of(t * subs + out_a, 8), out_b), :] = total

    loop(subs, settle, start=out_a)
    for copy in (
        *tables(), *lead_tokens(), *rest_tokens(), *forward_tokens(), *mix_far(), *mix_pure(), *mix_sum()
    ):
        copy.wait_send()

    @functools.partial(loop, MOST, unroll=1)
    def _(c):
        for copy in (plane_a(c), plane_b(c), return_a(c), return_b(c)):
            copy.wait_send()
        for group in (lead, rest, forward, scatter_far, scatter_pure, scatter_sum):
            for copy in group(c):
                copy.wait_send()


def per_device(tokens, routes, scores, gate_proj, up_proj, down_proj):
    plane = lax.axis_size("node") * (lax.axis_size("local") // SHARDS)
    count, wide = tokens.shape
    depth, hidden = gate_proj.shape[1:]
    block = wide // PARTS
    subs, step_subs = wide // LANES, block // LANES
    in_a, in_b = (PARTS - LATE_IN) * step_subs, LATE_IN * step_subs
    out_a, out_b = (PARTS - LATE_OUT) * step_subs, LATE_OUT * step_subs
    dma = pltpu.SemaphoreType.DMA
    vmem, smem, hbm = pltpu.VMEM, pltpu.SMEM, pl.ANY
    return pl.pallas_call(
        functools.partial(kernel, plane, count, block),
        out_shape=jax.ShapeDtypeStruct((count, wide), bf16),
        in_specs=[pl.BlockSpec(memory_space=m) for m in (vmem, vmem, vmem, hbm, hbm, hbm)],
        out_specs=pl.BlockSpec(memory_space=vmem),
        scratch_shapes=[
            vmem((depth, hidden), bf16),
            vmem((depth, hidden), bf16),
            vmem((hidden, depth), bf16),
            vmem((8, LANES), jnp.int32),
            vmem((8, LANES), f32),
            vmem((SHARDS, 8, LANES), jnp.int32),
            vmem((SHARDS, 8, LANES), f32),
            smem((SHARDS, 8, LANES), jnp.int32),
            smem((SHARDS, 8, LANES), f32),
            vmem((SHARDS, count, in_b, LANES), bf16),
            vmem((count, in_a, LANES), bf16),
            vmem((MOST, plane, in_a, LANES), bf16),
            vmem((MOST, plane, SHARDS, in_b, LANES), bf16),
            vmem((MOST, plane, in_a, LANES), bf16),
            vmem((MOST, plane, SHARDS, in_b, LANES), bf16),
            vmem((MOST, SHARDS, plane, in_a * LANES), bf16),
            vmem((SHARDS * plane, in_b * LANES), bf16),
            vmem((MOST, SHARDS, plane, out_a * LANES), bf16),
            vmem((MOST, 2, plane // 2, out_a * LANES), bf16),
            vmem((MOST, 2, plane, out_a * LANES), bf16),
            vmem((MOST, plane, out_a, LANES), bf16),
            vmem((MOST, plane, SHARDS, out_b, LANES), bf16),
            vmem((MOST, plane, out_a, LANES), bf16),
            vmem((MOST, plane, SHARDS, out_b, LANES), bf16),
            vmem((SHARDS, count, out_b, LANES), bf16),
            vmem((2, count // 2, out_b, LANES), bf16),
            vmem((2, count, out_b, LANES), bf16),
            vmem((max(plane * max(in_a, out_a, SHARDS * in_b, SHARDS * out_b), count * subs), LANES), f32),
            vmem((SHARDS * plane, 2 * hidden), f32),
            vmem((SHARDS * plane, hidden), bf16),
            dma((3,)),
            dma((3, 2)), dma((3, 2)), dma((8,)),
            dma((2, 2)), dma((2, 2)),
            dma((2,)), dma((2,)),
            dma((MOST,)), dma((MOST,)),
            dma((MOST,)), dma((MOST,)),
            dma((MOST, 2, 2)), dma((MOST, 2, 2)),
            dma((MOST, 2)), dma((MOST, 2)),
            dma((MOST, 2)), dma((MOST, 2)),
            dma((MOST, 2, 2)), dma((MOST, 2, 2)),
            dma((MOST,)), dma((MOST,)),
            dma((MOST,)), dma((MOST,)),
            dma((2,)), dma((2,)),
            dma((2, 2)), dma((2, 2)),
        ],
        compiler_params=pltpu.CompilerParams(
            collective_id=0, has_side_effects=True, vmem_limit_bytes=67043328
        ),
    )(routes.T, scores.T, tokens, gate_proj, up_proj, down_proj)


def solution(mesh):
    both = ("node", "local")
    return jax.shard_map(
        per_device,
        mesh=mesh,
        in_specs=(P(both, None),) * 3 + (P(both, None, None),) * 3,
        out_specs=P(both, None),
        check_vma=False,
    )
```

```python
import functools

import jax
import jax.numpy as jnp
from jax import lax
from jax.experimental import pallas as pl
from jax.experimental.pallas import tpu as pltpu
from jax.sharding import PartitionSpec as P

MESH = pl.DeviceIdType.MESH
SHARDS = 4
SCALE = 2.827
MOST = 5
LANES = 128
LATE_IN = 2
LATE_OUT = 3
PARTS = 7
UNROLL = 4
f32, bf16 = jnp.float32, jnp.bfloat16


def kernel(
    plane, count, block,
    routes_ref, scores_ref, tok_ref, gate_hbm, up_hbm, down_hbm,
    out_ref,
    w_gate, w_up, w_down, itab_in, ftab_in, itab_v, ftab_v, itab, ftab, tok_all, tok_a, sent_a, sent_b, got_a, got_b, x_a, x_b, part,
    half_in, full_in, back_a, back_b, home_a, home_b, mix, mix_half, mix_full, wide32, acc, hid,
    w_sem, tab_s, tab_r, tab_l, tok_s, tok_r, tfw_s, tfw_r, pa_s, pa_r, pb_s, pb_r, ag_s, ag_r, fw_s, fw_r,
    rh_s, rh_r, rf_s, rf_r, ba_s, ba_r, bb_s, bb_r, mh_s, mh_r, mf_s, mf_r,
):
    node, local = lax.axis_index("node"), lax.axis_index("local")
    ys = lax.axis_size("local") // SHARDS
    y, z = local // SHARDS, local % SHARDS
    me = node * ys + y
    nxt, far, prv = [(z + d) % SHARDS for d in (1, 2, 3)]
    nxt_dev, far_dev, prv_dev = [(node, y * SHARDS + q) for q in (nxt, far, prv)]
    z_devs = (nxt_dev, far_dev, prv_dev)
    hidden = w_gate.shape[1]
    step_subs = block // LANES
    subs = PARTS * step_subs
    in_a, in_b = (PARTS - LATE_IN) * step_subs, LATE_IN * step_subs
    out_a, out_b = (PARTS - LATE_OUT) * step_subs, LATE_OUT * step_subs
    half, half_t = plane // 2, count // 2
    rows = SHARDS * plane
    low, high = pl.ds(0, half), pl.ds(half, half)

    def loop(n, body, start=0, unroll=UNROLL):
        def wrapped(i, carry):
            body(i)
            return carry

        lax.fori_loop(start, n, wrapped, 0, unroll=unroll)

    w_copies = [
        pltpu.make_async_copy(gate_hbm.at[0], w_gate, w_sem.at[0]),
        pltpu.make_async_copy(up_hbm.at[0], w_up, w_sem.at[1]),
        pltpu.make_async_copy(down_hbm.at[0], w_down, w_sem.at[2]),
    ]
    for copy in w_copies:
        copy.start()

    chips = plane // (2 * ys)
    x, core = node // 2, node % 2

    def hops(step):
        return min(step[0], chips - step[0]) + min(step[2], ys - step[2])

    steps = [(dx, dc, dy) for dx in range(chips) for dc in range(2) for dy in range(ys)][1:]
    steps.sort(key=hops, reverse=True)
    peers = []
    for dx, dc, dy in steps:
        other_node, other_y = ((x + dx) % chips) * 2 + (core + dc) % 2, (y + dy) % ys
        peers.append((other_node * ys + other_y, (other_node, other_y * SHARDS + z)))

    barrier = pltpu.get_barrier_semaphore()

    for _, dev in peers:
        pl.semaphore_signal(barrier, inc=1, device_id=dev, device_id_type=MESH)

    for dev in z_devs:
        pl.semaphore_signal(barrier, inc=1, device_id=dev, device_id_type=MESH)

    def remote(src, dst, s_sem, r_sem, dev):
        return pltpu.make_async_remote_copy(
            src_ref=src, dst_ref=dst, send_sem=s_sem, recv_sem=r_sem, device_id=dev, device_id_type=MESH
        )

    def spread(src, dst, s_sem, r_sem, c):
        for other, dev in peers:
            remote(src.at[c, other], dst.at[c, me], s_sem.at[c], r_sem.at[c], dev).start()
        dst[c, me] = src[c, me]

    def spread_all(src, dst, s_sem, r_sem, c):
        some = pl.ds(0, plane - 1)
        return remote(src.at[c, some], dst.at[c, some], s_sem.at[c], r_sem.at[c], nxt_dev)

    plane_a = functools.partial(spread_all, sent_a, got_a, pa_s, pa_r)
    plane_b = functools.partial(spread_all, sent_b, got_b, pb_s, pb_r)
    return_a = functools.partial(spread_all, back_a, home_a, ba_s, ba_r)
    return_b = functools.partial(spread_all, back_b, home_b, bb_s, bb_r)

    def tables():
        copies = []
        for d, dev in enumerate(z_devs):
            copies.append(remote(itab_in, itab_v.at[z], tab_s.at[d, 0], tab_r.at[d, 0], dev))
            copies.append(remote(ftab_in, ftab_v.at[z], tab_s.at[d, 1], tab_r.at[d, 1], dev))
        return copies

    def both_ways(src_up, dst_up, src_dn, dst_dn, s_sem, r_sem):
        return (
            remote(src_up, dst_up, s_sem.at[0], r_sem.at[0], nxt_dev),
            remote(src_dn, dst_dn, s_sem.at[1], r_sem.at[1], prv_dev),
        )

    def same(ref_up, ref_dn, s_sem, r_sem):
        return both_ways(ref_up, ref_up, ref_dn, ref_dn, s_sem, r_sem)

    first, second = pl.ds(0, half_t), pl.ds(half_t, half_t)

    def lead_tokens():
        return same(tok_all.at[z, first], tok_all.at[z, second], tok_s.at[0], tok_r.at[0])

    def rest_tokens():
        return same(tok_all.at[z, second], tok_all.at[z, first], tok_s.at[1], tok_r.at[1])

    def forward_tokens():
        return same(tok_all.at[prv, first], tok_all.at[nxt, second], tfw_s, tfw_r)

    def lead(c):
        return same(x_a.at[c, z, low], x_a.at[c, z, high], ag_s.at[c, 0], ag_r.at[c, 0])

    def rest(c):
        return same(x_a.at[c, z, high], x_a.at[c, z, low], ag_s.at[c, 1], ag_r.at[c, 1])

    def forward(c):
        return same(x_a.at[c, prv, low], x_a.at[c, nxt, high], fw_s.at[c], fw_r.at[c])

    def scatter_far(c):
        return both_ways(
            part.at[c, far, low], half_in.at[c, 0], part.at[c, far, high], half_in.at[c, 1], rh_s.at[c], rh_r.at[c]
        )

    def scatter_pure(c):
        return both_ways(
            part.at[c, nxt, high], full_in.at[c, 0, high], part.at[c, prv, low], full_in.at[c, 1, low],
            rf_s.at[c, 0], rf_r.at[c, 0],
        )

    def scatter_sum(c):
        return both_ways(
            part.at[c, nxt, low], full_in.at[c, 0, low], part.at[c, prv, high], full_in.at[c, 1, high],
            rf_s.at[c, 1], rf_r.at[c, 1],
        )

    def mix_far():
        return both_ways(mix.at[far, first], mix_half.at[0], mix.at[far, second], mix_half.at[1], mh_s, mh_r)

    def mix_pure():
        return both_ways(
            mix.at[nxt, second], mix_full.at[0, second], mix.at[prv, first], mix_full.at[1, first],
            mf_s.at[0], mf_r.at[0],
        )

    def mix_sum():
        return both_ways(
            mix.at[nxt, first], mix_full.at[0, first], mix.at[prv, second], mix_full.at[1, second],
            mf_s.at[1], mf_r.at[1],
        )

    def start(*groups):
        for group in groups:
            for copy in group:
                copy.start()

    def await_in(*groups):
        for group in groups:
            for copy in group:
                copy.wait_recv()

    def fill_a(c):
        @functools.partial(loop, plane)
        def _(e):
            sent_a[c, e] = tok_a[itab[z, c // 4, (c % 4) * plane + e]]

    def launch_a(c):
        spread(sent_a, got_a, pa_s, pa_r, c)

    def launch_b(c):
        @functools.partial(loop, plane)
        def _(e):
            for q in range(SHARDS):
                sent_b[c, e, q] = tok_all[q, itab[q, c // 4, (c % 4) * plane + e]]

        spread(sent_b, got_b, pb_s, pb_r, c)

    def stage_a(c):
        plane_a(c).wait_recv()

        @functools.partial(loop, plane)
        def _(s):
            wide32[pl.ds(pl.multiple_of(s * in_a, 8), in_a), :] = got_a[c, s].astype(f32)

        @functools.partial(loop, in_a)
        def _(j):
            cols = pl.ds(pl.multiple_of(j * LANES, LANES), LANES)
            for s0 in range(0, plane, 16):
                pair = [wide32[pl.ds((s0 + d) * in_a + j, 8, stride=in_a), :] for d in (0, 8)]
                x_a[c, z, pl.ds(s0, 16), cols] = jnp.concatenate(pair, axis=0).astype(bf16)

        start(lead(c), rest(c))

    def stage_b(c):
        await_in(lead(c))
        start(forward(c))

    def stage_c(c):
        plane_b(c).wait_recv()

        @functools.partial(loop, plane)
        def _(p):
            for q in range(SHARDS):
                wide32[pl.ds(pl.multiple_of((q * plane + p) * in_b, 8), in_b), :] = got_b[c, p, q].astype(f32)

        @functools.partial(loop, in_b)
        def _(j):
            cols = pl.ds(pl.multiple_of(j * LANES, LANES), LANES)
            for s0 in range(0, rows, 16):
                pair = [wide32[pl.ds((s0 + d) * in_b + j, 8, stride=in_b), :] for d in (0, 8)]
                x_b[pl.ds(s0, 16), cols] = jnp.concatenate(pair, axis=0).astype(bf16)

        acc[...] = jnp.zeros_like(acc)

        def contract(rows_k, span):
            acc[:, :hidden] += jnp.dot(rows_k, w_gate[span, :], preferred_element_type=f32)
            acc[:, hidden:] += jnp.dot(rows_k, w_up[span, :], preferred_element_type=f32)

        @functools.partial(loop, LATE_IN, unroll=1)
        def _(k):
            here = pl.ds(pl.multiple_of(k * block, LANES), block)
            contract(x_b[:, here], pl.ds(pl.multiple_of((PARTS - LATE_IN + k) * block, LANES), block))

        await_in(rest(c), forward(c))

        @functools.partial(loop, PARTS - LATE_IN, unroll=1)
        def _(k):
            here = pl.ds(pl.multiple_of(k * block, LANES), block)
            contract(x_a[c, :, :, here].reshape(rows, block), here)

        gate = acc[:, :hidden]
        hid[...] = (gate / (1.0 + jnp.exp(-gate)) * acc[:, hidden:]).astype(bf16)

        @functools.partial(loop, LATE_OUT, unroll=1)
        def _(k):
            span = pl.ds(pl.multiple_of((PARTS - LATE_OUT + k) * block, LANES), block)
            value = jnp.dot(hid[...], w_down[:, span], preferred_element_type=f32)
            for j in range(step_subs):
                for s0 in range(0, rows, 8):
                    wide32[pl.ds(s0 * out_b + k * step_subs + j, 8, stride=out_b), :] = (
                        value[s0:s0 + 8, j * LANES:(j + 1) * LANES]
                    )

        @functools.partial(loop, plane)
        def _(p):
            for q in range(SHARDS):
                span = pl.ds(pl.multiple_of((q * plane + p) * out_b, 8), out_b)
                back_b[c, p, q] = wide32[span, :].astype(bf16)

        spread(back_b, home_b, bb_s, bb_r, c)

        @functools.partial(loop, PARTS - LATE_OUT, unroll=1)
        def _(k):
            span = pl.ds(pl.multiple_of(k * block, LANES), block)
            value = jnp.dot(hid[...], w_down[:, span], preferred_element_type=f32)
            part[c, :, :, span] = value.astype(bf16).reshape(SHARDS, plane, block)

        start(scatter_far(c), scatter_pure(c))

    def stage_e(c):
        await_in(scatter_far(c))
        for side, owner, span in ((0, nxt, low), (1, prv, high)):
            mine = part[c, owner, span].astype(f32)
            part[c, owner, span] = (mine + half_in[c, side].astype(f32)).astype(bf16)
        start(scatter_sum(c))

    def stage_f(c):
        await_in(scatter_pure(c), scatter_sum(c))

        @functools.partial(loop, out_a)
        def _(j):
            cols = pl.ds(pl.multiple_of(j * LANES, LANES), LANES)
            for s0 in range(0, plane, 16):
                span = pl.ds(s0, 16)
                value = part[c, z, span, cols].astype(f32)
                value = value + full_in[c, 0, span, cols].astype(f32)
                value = value + full_in[c, 1, span, cols].astype(f32)
                for d in (0, 8):
                    wide32[pl.ds((s0 + d) * out_a + j, 8, stride=out_a), :] = value[d:d + 8]

        @functools.partial(loop, plane)
        def _(s):
            back_a[c, s] = wide32[pl.ds(pl.multiple_of(s * out_a, 8), out_a), :].astype(bf16)

        spread(back_a, home_a, ba_s, ba_r, c)

    def weighted(source, q, t, subs, pick):
        total = jnp.zeros((subs, LANES), f32)
        for k in range(2):
            spot = itab[q, 2 + k, t]
            total = total + ftab[q, k, t] * pick(source, spot // plane, spot % plane)
        return total

    def mix_one(q):
        @functools.partial(loop, count)
        def _(t):
            take = lambda ref, c, e: ref[c, e, q].astype(f32)
            mix[q, t] = weighted(home_b, q, t, out_b, take).astype(bf16)

    def own_tables():
        routes, scores = routes_ref[...], scores_ref[...]
        expert = lax.broadcasted_iota(jnp.int32, (plane, count), 0)
        firsts, seconds = expert == routes[0:1, :], expert == routes[1:2, :]
        named = jnp.where(firsts | seconds, 1, 0)
        token = lax.broadcasted_iota(jnp.int32, (plane, count), 1)
        rank = jnp.zeros((plane, count), jnp.int32)
        for t in range(count - 1):
            rank = rank + jnp.where(token > t, named[:, t:t + 1], 0)
        spot = jnp.minimum(rank, MOST - 1) * plane + expert
        itab_in[...] = jnp.zeros_like(itab_in)
        ftab_in[...] = jnp.zeros_like(ftab_in)
        lane = lax.broadcasted_iota(jnp.int32, (plane, LANES), 1)
        sub = lax.broadcasted_iota(jnp.int32, (plane, LANES), 0)
        for row, slots in ((0, range(4)), (1, range(4, MOST))):
            spread_out = jnp.zeros((plane, LANES), jnp.int32)
            for c in slots:
                pick = jnp.sum(jnp.where(rank == c, named * token, 0), axis=1, keepdims=True)
                spread_out = spread_out + jnp.where(lane == sub + (c % 4) * plane, pick, 0)
            itab_in[row:row + 1, :] = jnp.sum(spread_out, axis=0, keepdims=True)
        weights = (SCALE * scores / (scores[0:1, :] + scores[1:2, :])).astype(bf16).astype(f32)
        for k, match in enumerate((firsts, seconds)):
            where = jnp.sum(jnp.where(match, spot, 0), axis=0, keepdims=True)
            itab_in[2 + k:3 + k, 0:count] = where
            ftab_in[k:k + 1, 0:count] = weights[k:k + 1, :]

    def unpack(j):
        cols = pl.ds(pl.multiple_of(j * LANES, LANES), LANES)
        for t0 in range(0, count, 16):
            value = tok_ref[pl.ds(t0, 16), cols].astype(f32)
            for d in (0, 8):
                wide32[pl.ds((t0 + d) * subs + j, 8, stride=subs), :] = value[d:d + 8]

    loop(subs, unpack, start=in_a)

    @functools.partial(loop, count)
    def _(t):
        tok_all[z, t] = wide32[pl.ds(pl.multiple_of(t * subs + in_a, 8), in_b), :].astype(bf16)

    own_tables()
    pl.semaphore_wait(barrier, plane + 2)
    start(lead_tokens(), rest_tokens())
    own_moves = [
        pltpu.make_async_copy(itab_in, itab.at[z], tab_l.at[0]),
        pltpu.make_async_copy(ftab_in, ftab.at[z], tab_l.at[1]),
    ]
    for move in own_moves:
        move.start()
    loop(in_a, unpack)

    @functools.partial(loop, count)
    def _(t):
        tok_a[t] = wide32[pl.ds(pl.multiple_of(t * subs, 8), in_a), :].astype(bf16)

    for move in own_moves:
        move.wait()
    fill_a(0)
    for copy in tables():
        copy.start()
    launch_a(0)
    for c in range(1, MOST):
        fill_a(c)
        if c < 3:
            launch_a(c)
    await_in(lead_tokens())
    start(forward_tokens())

    def ready():
        for copy in tables():
            copy.wait_recv()
        moves = []
        for d, q in enumerate((nxt, far, prv)):
            moves.append(pltpu.make_async_copy(itab_v.at[q], itab.at[q], tab_l.at[2 + 2 * d]))
            moves.append(pltpu.make_async_copy(ftab_v.at[q], ftab.at[q], tab_l.at[3 + 2 * d]))
        for move in moves:
            move.start()
        for move in moves:
            move.wait()
        await_in(rest_tokens(), forward_tokens())
        for copy in w_copies:
            copy.wait()

    def late(c):
        launch_b(c)

        @pl.when(c + 3 < MOST)
        def _():
            launch_a(c + 3)

    stages = ((stage_a, 0), (late, 1), (stage_b, 1), (stage_c, 2), (stage_e, 3), (stage_f, 4))

    def run(s, skip_last=False):
        @pl.when(s == 1)
        def _():
            ready()

        for stage, lag in stages:
            c = s - lag

            @pl.when((c >= 0) & (c < MOST))
            def _(stage=stage, c=c):
                stage(c)

    loop(MOST + 2, run, unroll=1)
    stage_e(MOST - 1)

    @functools.partial(loop, MOST, unroll=1)
    def _(c):
        return_b(c).wait_recv()

    mix_one(far)
    start(mix_far())
    stage_f(MOST - 2)
    mix_one(nxt)
    mix_one(prv)
    start(mix_pure())
    stage_f(MOST - 1)
    mix_one(z)
    await_in(mix_far())
    for side, owner, begin in ((0, nxt, 0), (1, prv, half_t)):
        @functools.partial(loop, half_t)
        def _(t):
            mix[owner, begin + t] = (mix[owner, begin + t].astype(f32) + mix_half[side, t].astype(f32)).astype(bf16)

    start(mix_sum())

    @functools.partial(loop, MOST, unroll=1)
    def _(c):
        return_a(c).wait_recv()

    @functools.partial(loop, count)
    def _(t):
        take = lambda ref, c, e: ref[c, e].astype(f32)
        wide32[pl.ds(pl.multiple_of(t * subs, 8), out_a), :] = weighted(home_a, z, t, out_a, take)

    def settle(j):
        cols = pl.ds(pl.multiple_of(j * LANES, LANES), LANES)
        for t0 in range(0, count, 16):
            pair = [wide32[pl.ds((t0 + d) * subs + j, 8, stride=subs), :] for d in (0, 8)]
            out_ref[pl.ds(t0, 16), cols] = jnp.concatenate(pair, axis=0).astype(bf16)

    loop(out_a, settle)
    await_in(mix_pure(), mix_sum())

    @functools.partial(loop, count)
    def _(t):
        total = mix[z, t].astype(f32) + mix_full[0, t].astype(f32) + mix_full[1, t].astype(f32)
        wide32[pl.ds(pl.multiple_of(t * subs + out_a, 8), out_b), :] = total

    loop(subs, settle, start=out_a)
    for copy in (
        *tables(), *lead_tokens(), *rest_tokens(), *forward_tokens(), *mix_far(), *mix_pure(), *mix_sum()
    ):
        copy.wait_send()

    @functools.partial(loop, MOST, unroll=1)
    def _(c):
        for copy in (plane_a(c), plane_b(c), return_a(c), return_b(c)):
            copy.wait_send()
        for group in (lead, rest, forward, scatter_far, scatter_pure, scatter_sum):
            for copy in group(c):
                copy.wait_send()


def per_device(tokens, routes, scores, gate_proj, up_proj, down_proj):
    plane = lax.axis_size("node") * (lax.axis_size("local") // SHARDS)
    count, wide = tokens.shape
    depth, hidden = gate_proj.shape[1:]
    block = wide // PARTS
    subs, step_subs = wide // LANES, block // LANES
    in_a, in_b = (PARTS - LATE_IN) * step_subs, LATE_IN * step_subs
    out_a, out_b = (PARTS - LATE_OUT) * step_subs, LATE_OUT * step_subs
    dma = pltpu.SemaphoreType.DMA
    vmem, smem, hbm = pltpu.VMEM, pltpu.SMEM, pl.ANY
    return pl.pallas_call(
        functools.partial(kernel, plane, count, block),
        out_shape=jax.ShapeDtypeStruct((count, wide), bf16),
        in_specs=[pl.BlockSpec(memory_space=m) for m in (vmem, vmem, vmem, hbm, hbm, hbm)],
        out_specs=pl.BlockSpec(memory_space=vmem),
        scratch_shapes=[
            vmem((depth, hidden), bf16),
            vmem((depth, hidden), bf16),
            vmem((hidden, depth), bf16),
            vmem((8, LANES), jnp.int32),
            vmem((8, LANES), f32),
            vmem((SHARDS, 8, LANES), jnp.int32),
            vmem((SHARDS, 8, LANES), f32),
            smem((SHARDS, 8, LANES), jnp.int32),
            smem((SHARDS, 8, LANES), f32),
            vmem((SHARDS, count, in_b, LANES), bf16),
            vmem((count, in_a, LANES), bf16),
            vmem((MOST, plane, in_a, LANES), bf16),
            vmem((MOST, plane, SHARDS, in_b, LANES), bf16),
            vmem((MOST, plane, in_a, LANES), bf16),
            vmem((MOST, plane, SHARDS, in_b, LANES), bf16),
            vmem((MOST, SHARDS, plane, in_a * LANES), bf16),
            vmem((SHARDS * plane, in_b * LANES), bf16),
            vmem((MOST, SHARDS, plane, out_a * LANES), bf16),
            vmem((MOST, 2, plane // 2, out_a * LANES), bf16),
            vmem((MOST, 2, plane, out_a * LANES), bf16),
            vmem((MOST, plane, out_a, LANES), bf16),
            vmem((MOST, plane, SHARDS, out_b, LANES), bf16),
            vmem((MOST, plane, out_a, LANES), bf16),
            vmem((MOST, plane, SHARDS, out_b, LANES), bf16),
            vmem((SHARDS, count, out_b, LANES), bf16),
            vmem((2, count // 2, out_b, LANES), bf16),
            vmem((2, count, out_b, LANES), bf16),
            vmem((max(plane * max(in_a, out_a, SHARDS * in_b, SHARDS * out_b), count * subs), LANES), f32),
            vmem((SHARDS * plane, 2 * hidden), f32),
            vmem((SHARDS * plane, hidden), bf16),
            dma((3,)),
            dma((3, 2)), dma((3, 2)), dma((8,)),
            dma((2, 2)), dma((2, 2)),
            dma((2,)), dma((2,)),
            dma((MOST,)), dma((MOST,)),
            dma((MOST,)), dma((MOST,)),
            dma((MOST, 2, 2)), dma((MOST, 2, 2)),
            dma((MOST, 2)), dma((MOST, 2)),
            dma((MOST, 2)), dma((MOST, 2)),
            dma((MOST, 2, 2)), dma((MOST, 2, 2)),
            dma((MOST,)), dma((MOST,)),
            dma((MOST,)), dma((MOST,)),
            dma((2,)), dma((2,)),
            dma((2, 2)), dma((2, 2)),
        ],
        compiler_params=pltpu.CompilerParams(
            collective_id=0, has_side_effects=True, vmem_limit_bytes=67043328
        ),
    )(routes.T, scores.T, tokens, gate_proj, up_proj, down_proj)


def solution(mesh):
    both = ("node", "local")
    return jax.shard_map(
        per_device,
        mesh=mesh,
        in_specs=(P(both, None),) * 3 + (P(both, None, None),) * 3,
        out_specs=P(both, None),
        check_vma=False,
    )
```
